32 devices in a mesh: pts: 8 (over z, y), cent: 4 (over x, core).
Axes of the slice: x: 2, y: 2, z: 4, core: 2. Of those that a mesh axis runs over, the one named last changes fastest.
Arguments:
- points: bfloat16 [65536, 512], P(('pts', 'cent')), may hold values from -128 to 128
- centroids: bfloat16 [8192, 512], P('pts'), may hold values from -32 to 32
- candidates: int32 [4096, 2], P(('pts', 'cent')), may hold values from 0 to 31, all different within a row; in each aligned block of 128 rows (0 to 127, 128 to 255, ...) at most 9 rows name the same one
Outputs:
- new_centroids: bfloat16 [8192, 512], P('pts')
- point_lse: float32 [65536], P(('pts', 'cent'))
The draws below stay inside these ranges and needn't reach their ends.
Inputs may be any that keep to these rules, and one draw needn't show every extreme that they name: `candidates`: within the 128 point blocks of one device, no centroid block is named more than 9 times; the two ids of a point block differ.
All inputs are finite; a program needn't handle non-finite values.
Results may differ from the reference program's by a relative error of at most 0.006.
Values may be sent and summed in bfloat16 or wider, within the bound.
A program may use at most 64 MiB of HBM per device.

```python
import math
import jax
import jax.numpy as jnp
import numpy as np
from jax import lax

D = 512
CB = 256
PB = 16
PBD = 128
ITERS = 2
NCB = 32
K = 8192
CAP = 9
NPB = 4096
NPTS = 65536


def draw_centroids(key, part):
    values = jnp.clip(jax.random.normal(jax.random.fold_in(key, 11), (K, D), jnp.float32), -6.0, 6.0)
    return jnp.clip(values, -32.0, 32.0).astype(jnp.bfloat16)


def draw_points(key, part):
    values = jnp.clip(jax.random.normal(jax.random.fold_in(key, 17), (NPTS, D), jnp.float32), -6.0, 6.0)
    return jnp.clip(values, -128.0, 128.0).astype(jnp.bfloat16)


def deal_out(rng, own, number, rows, amount, top, reach, skew):
    ranking = jax.random.permutation(rng, amount)
    heavy_load, ordinary = shares(amount, rows * top, reach, skew, True), shares(amount, rows * top, reach, skew, False)
    places = jnp.arange(amount)

    def named(tallies, turn):
        used = int((tallies > 0).sum())
        fixed = max(1, used // 4)
        passed = fixed + (places - fixed + turn * (used - fixed)) % max(1, amount - fixed)
        return jnp.zeros((amount,), jnp.int32).at[ranking[jnp.where(places < fixed, places, passed)]].set(jnp.asarray(tallies, jnp.int32))

    tallies = jnp.where(number % 4 == 0, named(heavy_load, number // 4), named(ordinary, number - number // 4 - 1))
    mixed = jax.random.permutation(jax.random.fold_in(own, 3), amount)
    donor, receiver = mixed[0:amount // 2 * 2:2], mixed[1:amount // 2 * 2:2]
    room = jnp.minimum(tallies[donor] - 1, reach - tallies[receiver]) // 2
    room = jnp.where((donor == ranking[0]) | (receiver == ranking[0]) | (tallies[receiver] == 0), 0, jnp.maximum(room, 0))
    passed = jax.random.randint(jax.random.fold_in(own, 4), (amount // 2,), 0, 1 << 20) % (room + 1)
    tallies = tallies.at[donor].add(-passed).at[receiver].add(passed)
    items = jnp.searchsorted(jnp.cumsum(tallies), jnp.arange(rows * top), side="right").astype(jnp.int32)
    grid = items.reshape(top, rows).T
    grid = grid[jax.random.permutation(jax.random.fold_in(own, 1), rows)]
    turn = jax.random.randint(jax.random.fold_in(own, 2), (rows, 1), 0, top)
    return jnp.take_along_axis(grid, (jnp.arange(top)[None, :] + turn) % top, axis=1)


def shares(number_of, total, limit, lean, full):
    loads = [(1 << 20) // math.isqrt(standing ** lean) + 1 for standing in range(1, number_of + 1)]
    largest = limit if full else min(limit, max(-(-total // number_of), total * loads[0] // sum(loads)))
    least = 1 if total - largest >= number_of - 1 else 0
    holding, surplus = [largest] + [least] * (number_of - 1), total - largest - least * (number_of - 1)
    while surplus > 0:
        free = [i for i in range(1, number_of) if holding[i] < largest] or [i for i in range(1, number_of) if holding[i] < limit]
        pool, budget = sum([loads[i] for i in free]), surplus
        for i in free:
            extra = min(limit - holding[i], max(1, budget * loads[i] // pool), surplus)
            holding[i] = holding[i] + extra
            surplus = surplus - extra
    return np.array(holding)


def setup_inputs(seed: int = 0) -> dict:
    key_list = jax.random.split(jax.random.key(seed), 4)
    points = draw_points(jax.random.fold_in(key_list[3], 71), 0)
    centroids = draw_centroids(jax.random.fold_in(key_list[3], 71), 0)
    candidates_keys = jax.random.split(jax.random.fold_in(key_list[2], 1), NPB // PBD)
    candidates_turns = jax.random.permutation(jax.random.fold_in(key_list[2], 3), NPB // PBD)
    candidates = jax.vmap(lambda own, number: deal_out(jax.random.fold_in(key_list[2], 2), own, number, PBD, NCB, 2, CAP, 2))(candidates_keys, candidates_turns).reshape((NPB, 2))
    return dict(points=points, centroids=centroids, candidates=candidates)


def stable_lse(scores, reduce_axis):
    highest = lax.optimization_barrier(jnp.max(scores, axis=reduce_axis, keepdims=True))
    summed = lax.optimization_barrier(jnp.sum(jnp.exp(scores - highest), axis=reduce_axis))
    return jnp.squeeze(highest, reduce_axis) + jnp.log(summed)

def em_round(points, current, candidates):
    inverse_root = 1.0 / math.sqrt(D)
    group_count = candidates.shape[0] // PBD
    grouped = points.reshape(group_count, PBD, PB, D)
    picked = candidates.reshape(group_count, PBD, 2)
    centre_table = current.reshape(NCB, CB, D)
    centre_norms = lax.optimization_barrier(jnp.sum(jnp.square(centre_table.astype(jnp.float32)), axis=2))

    def visit_group(running, element):
        weighted, masses = running
        group_rows, group_ids = element
        chosen = centre_table[group_ids].astype(jnp.float32)
        products = jnp.einsum('gpd,gjmd->gjpm', group_rows.astype(jnp.float32), chosen)
        scores = inverse_root * (2.0 * products - centre_norms[group_ids][:, :, None, :])
        partial_value = stable_lse(scores, 3)
        point_lse = stable_lse(partial_value, 1)
        weights = jnp.exp(scores - point_lse[:, None, :, None])
        rounded = lax.optimization_barrier(weights.astype(jnp.bfloat16)).astype(jnp.float32)
        contribution = jnp.einsum('gjpm,gpd->gjmd', rounded, group_rows.astype(jnp.float32))
        weighted = weighted.at[group_ids].add(contribution)
        masses = masses.at[group_ids].add(lax.optimization_barrier(jnp.sum(weights, axis=2)))
        return ((weighted, masses), point_lse)
    start_sums = jnp.zeros((NCB, CB, D), jnp.float32)
    start_mass = jnp.zeros((NCB, CB), jnp.float32)
    (weighted, masses), point_lse = lax.scan(visit_group, (start_sums, start_mass), (grouped, picked))
    return (weighted.reshape(K, D), masses.reshape(K), point_lse.reshape(-1))

def reference(points, centroids, candidates):
    current = centroids
    point_lse = jnp.zeros((NPTS,), jnp.float32)
    for iteration in range(ITERS):
        weighted, masses, point_lse = em_round(points, current, candidates)
        current = ((weighted + current.astype(jnp.float32)) / (masses[:, None] + 1.0)).astype(jnp.bfloat16)
    return (current, point_lse)
```

```python
import functools
import math

import jax
import jax.numpy as jnp
from jax import lax
from jax.experimental import pallas as pl
from jax.experimental.pallas import tpu as pltpu
from jax.sharding import PartitionSpec as P

CB = 256
PB = 16
ITERS = 2
LANES = 128
GROUP = LANES // PB
CHUNKS = 4
MESH = pl.DeviceIdType.MESH
FAR = 1e30


class Plan:
    def __init__(self, pts, cent, point_blocks, width):
        self.pts, self.cent, self.blocks, self.width = pts, cent, point_blocks, width
        self.half = pts // 2
        self.spots = self.half * cent
        self.total = 2 * self.spots
        self.cap = max(2, 2 * point_blocks // self.total + 1)
        self.main = self.cap // GROUP * GROUP
        self.rem = self.cap - self.main
        self.main_rows = self.main // GROUP
        self.rows = self.main_rows + (self.rem > 0)
        self.share = GROUP // self.rem if self.rem else 1
        self.slots = self.total * self.cap
        self.held = self.spots * self.cap
        self.groups = self.held // GROUP
        self.tiles = self.groups // 2
        self.tile_blocks = 2 * GROUP
        assert GROUP % max(self.rem, 1) == 0 and 2 * self.rows <= 8
        assert self.spots & (self.spots - 1) == 0 and self.held % self.tile_blocks == 0

    def pair_order(self):
        pairs = self.spots // 2
        if pairs == 8:
            return (7, 3, 4, 5, 2, 1, 6, 0)
        return tuple(reversed(range(pairs)))


def flip(value, mask):
    out, bit = 0, 1
    while bit <= mask or bit == 1:
        here = (value // bit) % 2
        out = out + bit * ((1 - here) if mask & bit else here)
        bit *= 2
    return out + (value // bit) * bit


def split3(x):
    hi = x.astype(jnp.bfloat16)
    left = x - hi.astype(jnp.float32)
    mid = left.astype(jnp.bfloat16)
    low = (left - mid.astype(jnp.float32)).astype(jnp.bfloat16)
    return jnp.concatenate([hi, mid, low], axis=1)


def pick_rows(onehot, packed):
    out = jnp.dot(onehot, packed, preferred_element_type=jnp.float32)
    return (out[:, :LANES] + out[:, LANES : 2 * LANES]) + out[:, 2 * LANES :]


def iota(shape, axis):
    return lax.broadcasted_iota(jnp.int32, shape, axis)


def to_column(row, start, size):
    parts = []
    for first in range(0, size, LANES):
        part = min(LANES, size - first)
        piece = row[:, start + first : start + first + LANES]
        same = iota((part, LANES), 0) == iota((part, LANES), 1)
        parts.append(jnp.sum(jnp.where(same, piece, 0.0), axis=1, keepdims=True))
    return jnp.concatenate(parts, axis=0)


def to_row(column):
    parts = []
    for first in range(0, column.shape[0], LANES):
        same = iota((LANES, LANES), 0) == iota((LANES, LANES), 1)
        parts.append(jnp.sum(jnp.where(same, column[first : first + LANES], 0.0), axis=0, keepdims=True))
    return jnp.concatenate(parts, axis=1)


def kernel(
    pn, inverse_root, home, table, points, cent_in, new_out, lse_out,
    stage, recv, cents, norms, escr, mrow, lrow, acc, macc,
    pick, pick_lane, back, fill,
    pmsg, pin, lmsg, lin, xout, xin, mout, min_, xout2, xin2, mout2, min2,
    main_s, main_r, rem_s, rem_r, cent_sem, cs, cr, ps, pr, ls, lr,
    xs, xr, ms, mr, x2s, x2r, m2s, m2r, fs, fr,
):
    p, c = lax.axis_index("pts"), lax.axis_index("cent")
    side = p // pn.half
    other = 1 - side
    q = (p % pn.half) * pn.cent + c
    Q = pn.spots

    def device(spot):
        return {"pts": side * pn.half + spot // pn.cent, "cent": spot % pn.cent}

    partner = {"pts": other * pn.half + p % pn.half, "cent": c}

    def remote(src, dst, send, recv_sem, to):
        return pltpu.make_async_remote_copy(
            src_ref=src, dst_ref=dst, send_sem=send, recv_sem=recv_sem,
            device_id=to, device_id_type=MESH,
        )

    barrier = pltpu.get_barrier_semaphore()
    for mask in range(1, Q):
        pl.semaphore_signal(barrier, inc=1, device_id=device(flip(q, mask)), device_id_type=MESH)
    pl.semaphore_signal(barrier, inc=1, device_id=partner, device_id_type=MESH)
    own_copy = pltpu.make_async_copy(cent_in.at[c], cents.at[side], cent_sem)
    own_copy.start()

    masks = [2 * pair + low for pair in pn.pair_order() for low in (0, 1)]

    def gather(mask):
        spot = flip(q, mask)
        for sel in range(2):
            first = (sel * Q + spot) * pn.cap

            @pl.loop(0, pn.cap)
            def _(t):
                stage[mask, sel, t] = points[home[first + t]]

    def gather_own():
        for sel in range(2):
            first = (sel * Q + q) * pn.cap
            if pn.main:
                @pl.loop(0, pn.main)
                def _(t):
                    recv[sel, q * pn.main + t] = points[home[first + t]]
            if pn.rem:
                @pl.loop(0, pn.rem)
                def _(t):
                    recv[sel, Q * pn.main + q * pn.rem + t] = points[home[first + pn.main + t]]

    def main_copy(mask, sel, spot_at):
        return remote(
            stage.at[mask, sel, pl.ds(0, pn.main)],
            recv.at[sel, pl.ds(spot_at * pn.main, pn.main)],
            main_s.at[mask, sel], main_r.at[spot_at, sel], device(flip(q, mask)),
        )

    def rem_copy(mask, sel, spot_at):
        return remote(
            stage.at[mask, sel, pl.ds(pn.main, pn.rem)],
            recv.at[sel, pl.ds(Q * pn.main + spot_at * pn.rem, pn.rem)],
            rem_s.at[mask, sel], rem_r.at[spot_at, sel], device(flip(q, mask)),
        )

    def send(mask):
        for sel in range(2):
            if pn.main:
                main_copy(mask, sel, q).start()
            if pn.rem:
                rem_copy(mask, sel, q).start()

    waiting = None
    for mask in masks:
        if mask:
            gather(mask)
            if waiting is None:
                pl.semaphore_wait(barrier, Q)
            else:
                send(waiting)
            waiting = mask
    own_copy.wait()
    send(waiting)
    cent_copy = remote(cents.at[side], cents.at[side], cs, cr, partner)
    cent_copy.start()
    cent_wait = remote(cents.at[other], cents.at[other], cs, cr, partner)
    gather_own()

    lanes = table[...].astype(jnp.float32)
    entries = 2 * pn.blocks
    entry_row = to_column(lanes[0:1], 0, entries)
    entry_lane = to_column(lanes[1:2], 0, entries)
    slot_home = to_column(lanes[2:3], 0, pn.slots)
    pick[...] = (entry_row == iota((entries, 8 * Q), 1).astype(jnp.float32)).astype(jnp.bfloat16)
    lane_group = (iota((entries, LANES), 1) // PB).astype(jnp.float32)
    pick_lane[...] = (entry_lane == lane_group).astype(jnp.float32)
    back[...] = (slot_home == iota((pn.slots, pn.blocks), 1).astype(jnp.float32)).astype(jnp.bfloat16)
    fill[...] = jnp.broadcast_to(jnp.where(slot_home < 0.0, FAR, 0.0), fill.shape)
    pmsg[...] = jnp.zeros_like(pmsg)
    lmsg[...] = jnp.zeros_like(lmsg)

    def set_norm(sel):
        wide = cents[sel].astype(jnp.float32)
        norms[sel] = jnp.broadcast_to(jnp.sum(wide * wide, axis=1, keepdims=True), (CB, LANES))

    def tile_rows(sel, tile):
        block = recv[sel, pl.ds(tile * pn.tile_blocks, pn.tile_blocks)]
        return block.reshape(pn.tile_blocks * PB, pn.width)

    def score_tile(sel, tile):
        products = lax.dot_general(
            cents[sel], tile_rows(sel, tile), (((1,), (1,)), ((), ())),
            preferred_element_type=jnp.float32,
        )
        out = []
        for h in range(2):
            scores = inverse_root * (2.0 * products[:, h * LANES : (h + 1) * LANES] - norms[sel])
            highest = jnp.max(scores, axis=0, keepdims=True)
            raised = jnp.exp(scores - highest)
            escr[sel, 2 * tile + h] = raised
            mrow[pl.ds(sel * pn.groups + 2 * tile + h, 1)] = highest
            out.append(highest + jnp.log(jnp.sum(raised, axis=0, keepdims=True)))
        return out

    def score_main(it, sel, tile):
        for h, part in enumerate(score_tile(sel, tile)):
            group = 2 * tile + h
            row = (group // pn.main_rows) * 8 + sel * pn.rows + group % pn.main_rows
            pmsg[it, pl.ds(row, 1)] = part

    main_tiles = Q * pn.main_rows // 2

    def score_rem(it, sel, tile):
        for h, part in enumerate(score_tile(sel, tile)):
            first = (2 * tile + h - Q * pn.main_rows) * pn.share
            for s in range(pn.share):
                row = (first + s) * 8 + sel * pn.rows + pn.main_rows
                pmsg[it, pl.ds(row, 1)] = part

    def score_all_rem(it, sel):
        @pl.loop(main_tiles, pn.tiles)
        def _(tile):
            score_rem(it, sel, tile)

    def trade(out, into, send_sem, recv_sem, it):
        into[it, pl.ds(q * 8, 8)] = out[it, pl.ds(q * 8, 8)]
        for mask in masks:
            if mask:
                spot = flip(q, mask)
                remote(
                    out.at[it, pl.ds(spot * 8, 8)], into.at[it, pl.ds(q * 8, 8)],
                    send_sem.at[it, mask], recv_sem.at[it, q], device(spot),
                ).start()
        for mask in masks:
            if mask:
                spot = flip(q, mask)
                copy = remote(
                    out.at[it, pl.ds(spot * 8, 8)], into.at[it, pl.ds(spot * 8, 8)],
                    send_sem.at[it, mask], recv_sem.at[it, spot], device(spot),
                )
                copy.wait()

    def combine(it):
        chosen = pick_rows(pick[...], split3(pin[it]))
        chosen = jnp.where(pick_lane[...] > 0.5, chosen, 0.0)
        step = LANES // 2
        while step >= PB:
            chosen = chosen + pltpu.roll(chosen, step, 1)
            step //= 2
        first, second = chosen[: pn.blocks], chosen[pn.blocks :]
        highest = jnp.maximum(first, second)
        lse = highest + jnp.log(jnp.exp(first - highest) + jnp.exp(second - highest))
        if it == ITERS - 1:
            grouped = lse.reshape(pn.blocks // GROUP, GROUP, LANES)
            shape = grouped.shape
            mine = iota(shape, 2) // PB == iota(shape, 1)
            lse_out[...] = jnp.sum(jnp.where(mine, grouped, 0.0), axis=1)
        spread = pick_rows(back[...], split3(lse)) + fill[...]
        lane = iota((2 * Q, LANES), 1) // PB
        for r in range(pn.rows):
            total = jnp.zeros((2 * Q, LANES), jnp.float32)
            for t in range(pn.cap):
                if (t // GROUP if t < pn.main else pn.main_rows) == r:
                    group = t % GROUP if t < pn.main else (q % pn.share) * pn.rem + t - pn.main
                    total = total + jnp.where(lane == group, spread[t * 2 * Q : (t + 1) * 2 * Q], 0.0)
            for sel in range(2):
                lmsg[it, pl.ds(sel * pn.rows + r, Q, stride=8)] = total[sel * Q : (sel + 1) * Q]

    def unpack(it):
        for sel in range(2):
            base = sel * pn.groups
            for r in range(pn.main_rows):
                rows = lin[it, pl.ds(sel * pn.rows + r, Q, stride=8)]
                if pn.main_rows == 1:
                    lrow[pl.ds(base, Q)] = rows
                else:
                    lrow[pl.ds(base + r, Q, stride=pn.main_rows)] = rows
            if pn.rem:
                rows = lin[it, pl.ds(sel * pn.rows + pn.main_rows, Q, stride=8)]
                joined = jnp.sum(rows.reshape(Q // pn.share, pn.share, LANES), axis=1)
                lrow[pl.ds(base + Q * pn.main_rows, Q // pn.share)] = joined

    def sum_up(sel):
        acc[...] = jnp.zeros_like(acc)
        macc[...] = jnp.zeros_like(macc)

        @pl.loop(0, pn.tiles)
        def _(tile):
            parts = []
            for h in range(2):
                row = sel * pn.groups + 2 * tile + h
                scale = jnp.exp(mrow[pl.ds(row, 1)] - lrow[pl.ds(row, 1)])
                weights = escr[sel, 2 * tile + h] * scale
                macc[...] += weights
                parts.append(weights.astype(jnp.bfloat16))
            acc[...] += jnp.dot(
                jnp.concatenate(parts, axis=1), tile_rows(sel, tile),
                preferred_element_type=jnp.float32,
            )

        return jnp.sum(macc[...], axis=1, keepdims=True)

    set_norm(side)
    cent_wait.wait_recv()
    set_norm(other)

    def wait_main(mask):
        spot = flip(q, mask)
        for sel in range(2):
            main_copy(mask, sel, spot).wait_recv()

    for pair in pn.pair_order()[-1:] + pn.pair_order()[:-1]:
        if pn.main:
            for low in (0, 1):
                if 2 * pair + low:
                    wait_main(2 * pair + low)
            if pn.main_rows == 1:
                tile = flip(q, 2 * pair) // 2

                @pl.loop(0, 2)
                def _(sel):
                    score_main(0, sel, tile)
    if pn.main_rows > 1:
        for sel in range(2):
            @pl.loop(0, main_tiles)
            def _(tile):
                score_main(0, sel, tile)
    if pn.rem:
        for mask in masks:
            if mask:
                for sel in range(2):
                    rem_copy(mask, sel, flip(q, mask)).wait_recv()
        for sel in range(2):
            score_all_rem(0, sel)
    trade(pmsg, pin, ps, pr, 0)
    combine(0)
    trade(lmsg, lin, ls, lr, 0)
    unpack(0)

    def x_copy(sel):
        return remote(xout.at[sel], xin.at[sel], xs.at[sel], xr.at[sel], partner)

    def m_copy(sel):
        return remote(mout.at[sel], min_.at[sel], ms.at[sel], mr.at[sel], partner)

    for sel in (other, side):
        mass = sum_up(sel)
        mout[sel] = jnp.broadcast_to(to_row(mass), (8, CB))
        xout[sel] = acc[...].astype(jnp.bfloat16)
        m_copy(sel).start()
        x_copy(sel).start()

    def renewed(sums, mass, old):
        return ((sums + old.astype(jnp.float32)) / (mass + 1.0)).astype(jnp.bfloat16)

    cent_copy.wait_send()
    for sel in (side, other):
        m_copy(sel).wait_recv()
        x_copy(sel).wait_recv()
        mass = to_column(mout[sel][0:1] + min_[sel][0:1], 0, CB)
        both = xout[sel].astype(jnp.float32) + xin[sel].astype(jnp.float32)
        cents[sel] = renewed(both, mass, cents[sel])
        set_norm(sel)
        if pn.main:
            @pl.loop(0, main_tiles)
            def _(tile):
                score_main(1, sel, tile)
        if pn.rem:
            score_all_rem(1, sel)

    trade(pmsg, pin, ps, pr, 1)
    combine(1)
    trade(lmsg, lin, ls, lr, 1)
    unpack(1)
    rows = CB // CHUNKS

    def x2_copy(k):
        part = pl.ds(k * rows, rows)
        return remote(xout2.at[part], xin2.at[part], x2s.at[k], x2r.at[k], partner)

    m2_copy = remote(mout2, min2, m2s, m2r, partner)
    mass = sum_up(other)
    mout2[...] = jnp.broadcast_to(to_row(mass), (8, CB))
    xout2[...] = acc[...].astype(jnp.bfloat16)
    m2_copy.start()
    for k in range(CHUNKS):
        x2_copy(k).start()
    mass = sum_up(side)
    m2_copy.wait_recv()
    mass = mass + to_column(min2[0:1], 0, CB)

    def f_copy(step, k, spot):
        part = new_out.at[spot, pl.ds(k * rows, rows)]
        to = {"pts": p, "cent": (c + step) % pn.cent}
        return remote(part, part, fs.at[step, k], fr.at[spot, k], to)

    for k in range(CHUNKS):
        part = pl.ds(k * rows, rows)
        x2_copy(k).wait_recv()
        sums = acc[part] + xin2[part].astype(jnp.float32)
        new_out[c, part] = renewed(sums, mass[k * rows : (k + 1) * rows], cents[side, part])
        for step in range(1, pn.cent):
            f_copy(step, k, c).start()

    for mask in masks:
        if mask:
            for sel in range(2):
                if pn.main:
                    main_copy(mask, sel, q).wait_send()
                if pn.rem:
                    rem_copy(mask, sel, q).wait_send()
    for sel in range(2):
        m_copy(sel).wait_send()
        x_copy(sel).wait_send()
    m2_copy.wait_send()
    for k in range(CHUNKS):
        x2_copy(k).wait_send()
        for step in range(1, pn.cent):
            f_copy(step, k, c).wait_send()
            f_copy(step, k, (c - step + pn.cent) % pn.cent).wait_recv()


def tables(pn, candidates):
    q = (lax.axis_index("pts") % pn.half) * pn.cent + lax.axis_index("cent")
    picked = candidates.T.reshape(-1)
    count = picked.shape[0]
    index = jnp.arange(count, dtype=jnp.int32)
    labels = jnp.arange(pn.total, dtype=jnp.int32)
    member = (picked[:, None] == labels[None, :]).astype(jnp.bfloat16)
    earlier = (index[None, :] < index[:, None]).astype(jnp.bfloat16)
    prior = jnp.dot(earlier, member, preferred_element_type=jnp.float32)
    turn = jnp.sum(prior * member.astype(jnp.float32), axis=1).astype(jnp.int32)
    place = picked * pn.cap + turn
    spot, sel = picked % pn.spots, picked // pn.spots
    in_main = turn < pn.main
    row = spot * 8 + sel * pn.rows + jnp.where(in_main, turn // GROUP, pn.main_rows)
    lane = jnp.where(in_main, turn % GROUP, (q % pn.share) * pn.rem + turn - pn.main)
    places = jnp.arange(pn.slots, dtype=jnp.int32)
    block = index % pn.blocks
    source = jnp.sum(jnp.where(place[:, None] == places[None, :], block[:, None] + 1, 0), axis=0) - 1
    by_turn = source.reshape(pn.total, pn.cap).T.reshape(-1)
    width = -(-max(count, pn.slots) // LANES) * LANES

    def row_of(values):
        return jnp.pad(values, (0, width - values.shape[0]))[None]

    rows = jnp.concatenate([row_of(row), row_of(lane), row_of(by_turn)], axis=0)
    table = jnp.pad(rows, ((0, 5), (0, 0)))
    return jnp.maximum(source, 0), table


def on_device(points, centroids, candidates):
    width = points.shape[1]
    pn = Plan(lax.axis_size("pts"), lax.axis_size("cent"), candidates.shape[0], width)
    assert centroids.shape[0] == pn.cent * CB
    home, table = tables(pn, candidates)
    Q, bf16, f32 = pn.spots, jnp.bfloat16, jnp.float32
    vmem = pl.BlockSpec(memory_space=pltpu.VMEM)
    dma = pltpu.SemaphoreType.DMA
    new, lse = pl.pallas_call(
        functools.partial(kernel, pn, 1.0 / math.sqrt(width)),
        out_shape=(
            jax.ShapeDtypeStruct((pn.cent, CB, width), bf16),
            jax.ShapeDtypeStruct((pn.blocks // GROUP, LANES), f32),
        ),
        in_specs=[pl.BlockSpec(memory_space=pltpu.SMEM), vmem, vmem, pl.BlockSpec(memory_space=pl.ANY)],
        out_specs=(vmem, vmem),
        scratch_shapes=[
            pltpu.VMEM((Q, 2, pn.cap, PB, width), bf16),
            pltpu.VMEM((2, pn.held, PB, width), bf16),
            pltpu.VMEM((2, CB, width), bf16),
            pltpu.VMEM((2, CB, LANES), f32),
            pltpu.VMEM((2, pn.groups, CB, LANES), f32),
            pltpu.VMEM((2 * pn.groups, LANES), f32),
            pltpu.VMEM((2 * pn.groups, LANES), f32),
            pltpu.VMEM((CB, width), f32),
            pltpu.VMEM((CB, LANES), f32),
            pltpu.VMEM((2 * pn.blocks, 8 * Q), bf16),
            pltpu.VMEM((2 * pn.blocks, LANES), f32),
            pltpu.VMEM((pn.slots, pn.blocks), bf16),
            pltpu.VMEM((pn.slots, LANES), f32),
            pltpu.VMEM((ITERS, 8 * Q, LANES), f32),
            pltpu.VMEM((ITERS, 8 * Q, LANES), f32),
            pltpu.VMEM((ITERS, 8 * Q, LANES), f32),
            pltpu.VMEM((ITERS, 8 * Q, LANES), f32),
            pltpu.VMEM((2, CB, width), bf16),
            pltpu.VMEM((2, CB, width), bf16),
            pltpu.VMEM((2, 8, CB), f32),
            pltpu.VMEM((2, 8, CB), f32),
            pltpu.VMEM((CB, width), bf16),
            pltpu.VMEM((CB, width), bf16),
            pltpu.VMEM((8, CB), f32),
            pltpu.VMEM((8, CB), f32),
            dma((Q, 2)), dma((Q, 2)), dma((Q, 2)), dma((Q, 2)),
            dma, dma, dma,
            dma((ITERS, Q)), dma((ITERS, Q)), dma((ITERS, Q)), dma((ITERS, Q)),
            dma((2,)), dma((2,)), dma((2,)), dma((2,)),
            dma((CHUNKS,)), dma((CHUNKS,)), dma, dma,
            dma((pn.cent, CHUNKS)), dma((pn.cent, CHUNKS)),
        ],
        compiler_params=pltpu.CompilerParams(
            collective_id=0, has_side_effects=True, vmem_limit_bytes=60 << 20
        ),
    )(home, table, points.reshape(pn.blocks, PB, width), centroids.reshape(pn.cent, CB, width))
    return new.reshape(centroids.shape), lse.reshape(-1)


def solution(mesh):
    return jax.shard_map(
        on_device,
        mesh=mesh,
        in_specs=(P(("pts", "cent"), None), P("pts", None), P(("pts", "cent"), None)),
        out_specs=(P("pts", None), P(("pts", "cent"))),
        check_vma=False,
    )
```

```python
import functools
import math

import jax
import jax.numpy as jnp
from jax import lax
from jax.experimental import pallas as pl
from jax.experimental.pallas import tpu as pltpu
from jax.sharding import PartitionSpec as P

CB = 256
PB = 16
ITERS = 2
LANES = 128
GROUP = LANES // PB
CHUNKS = 8
SPARE = 12 << 20
LOG2E = math.log2(math.e)
LN2 = math.log(2.0)
MESH = pl.DeviceIdType.MESH
FAR = 1e30


class Plan:
    def __init__(self, pts, cent, point_blocks, width):
        self.pts, self.cent, self.blocks, self.width = pts, cent, point_blocks, width
        self.half = pts // 2
        self.spots = self.half * cent
        self.total = 2 * self.spots
        self.cap = max(2, 2 * point_blocks // self.total + 1)
        self.main = self.cap // GROUP * GROUP
        self.rem = self.cap - self.main
        self.main_rows = self.main // GROUP
        self.rows = self.main_rows + (self.rem > 0)
        self.share = GROUP // self.rem if self.rem else 1
        self.slots = self.total * self.cap
        self.held = self.spots * self.cap
        self.groups = self.held // GROUP
        self.tiles = self.groups // 2
        self.tile_blocks = 2 * GROUP
        assert GROUP % max(self.rem, 1) == 0 and 2 * self.rows <= 8
        assert self.spots & (self.spots - 1) == 0 and self.held % self.tile_blocks == 0

    def pair_order(self):
        pairs = self.spots // 2
        if pairs == 8:
            return (7, 3, 4, 5, 2, 1, 6, 0)
        return tuple(reversed(range(pairs)))


def flip(value, mask):
    out, bit = 0, 1
    while bit <= mask or bit == 1:
        here = (value // bit) % 2
        out = out + bit * ((1 - here) if mask & bit else here)
        bit *= 2
    return out + (value // bit) * bit


def split3(x):
    hi = x.astype(jnp.bfloat16)
    left = x - hi.astype(jnp.float32)
    mid = left.astype(jnp.bfloat16)
    low = (left - mid.astype(jnp.float32)).astype(jnp.bfloat16)
    return jnp.concatenate([hi, mid, low], axis=1)


def pick_rows(onehot, packed):
    out = jnp.dot(onehot, packed, preferred_element_type=jnp.float32)
    return (out[:, :LANES] + out[:, LANES : 2 * LANES]) + out[:, 2 * LANES :]


def iota(shape, axis):
    return lax.broadcasted_iota(jnp.int32, shape, axis)


def to_column(row, start, size):
    parts = []
    for first in range(0, size, LANES):
        part = min(LANES, size - first)
        piece = row[:, start + first : start + first + LANES]
        same = iota((part, LANES), 0) == iota((part, LANES), 1)
        parts.append(jnp.sum(jnp.where(same, piece, 0.0), axis=1, keepdims=True))
    return jnp.concatenate(parts, axis=0)


def to_row(column):
    parts = []
    for first in range(0, column.shape[0], LANES):
        same = iota((LANES, LANES), 0) == iota((LANES, LANES), 1)
        parts.append(jnp.sum(jnp.where(same, column[first : first + LANES], 0.0), axis=0, keepdims=True))
    return jnp.concatenate(parts, axis=1)


def kernel(
    pn, inverse_root, home, table, points, cent_in, new_out, lse_out,
    stage, recv, cents, norms, escr, wscr, mrow, lrow, acc, macc,
    pick, pick_lane, back, fill,
    pmsg, pin, lmsg, lin, xout, xin, mout, min_, xout2, xin2, mout2, min2,
    main_s, main_r, rem_s, rem_r, cent_sem, cs, cr, ps, pr, ls, lr,
    xs, xr, ms, mr, x2s, x2r, m2s, m2r, fs, fr,
):
    p, c = lax.axis_index("pts"), lax.axis_index("cent")
    side = p // pn.half
    other = 1 - side
    q = (p % pn.half) * pn.cent + c
    Q = pn.spots

    def device(spot):
        return {"pts": side * pn.half + spot // pn.cent, "cent": spot % pn.cent}

    partner = {"pts": other * pn.half + p % pn.half, "cent": c}

    def remote(src, dst, send, recv_sem, to):
        return pltpu.make_async_remote_copy(
            src_ref=src, dst_ref=dst, send_sem=send, recv_sem=recv_sem,
            device_id=to, device_id_type=MESH,
        )

    barrier = pltpu.get_barrier_semaphore()
    for mask in range(1, Q):
        pl.semaphore_signal(barrier, inc=1, device_id=device(flip(q, mask)), device_id_type=MESH)
    pl.semaphore_signal(barrier, inc=1, device_id=partner, device_id_type=MESH)
    own_copy = pltpu.make_async_copy(cent_in.at[c], cents.at[side], cent_sem)
    own_copy.start()

    masks = [2 * pair + low for pair in pn.pair_order() for low in (0, 1)]

    def gather(mask):
        spot = flip(q, mask)
        for sel in range(2):
            first = (sel * Q + spot) * pn.cap

            @pl.loop(0, pn.cap, unroll=pn.cap)
            def _(t):
                stage[mask, sel, t] = points[home[first + t]]

    def gather_own():
        for sel in range(2):
            first = (sel * Q + q) * pn.cap
            if pn.main:
                @pl.loop(0, pn.main)
                def _(t):
                    recv[sel, q * pn.main + t] = points[home[first + t]]
            if pn.rem:
                @pl.loop(0, pn.rem)
                def _(t):
                    recv[sel, Q * pn.main + q * pn.rem + t] = points[home[first + pn.main + t]]

    def main_copy(mask, sel, spot_at):
        return remote(
            stage.at[mask, sel, pl.ds(0, pn.main)],
            recv.at[sel, pl.ds(spot_at * pn.main, pn.main)],
            main_s.at[mask, sel], main_r.at[spot_at, sel], device(flip(q, mask)),
        )

    def rem_copy(mask, sel, spot_at):
        return remote(
            stage.at[mask, sel, pl.ds(pn.main, pn.rem)],
            recv.at[sel, pl.ds(Q * pn.main + spot_at * pn.rem, pn.rem)],
            rem_s.at[mask, sel], rem_r.at[spot_at, sel], device(flip(q, mask)),
        )

    def send(mask):
        for sel in range(2):
            if pn.main:
                main_copy(mask, sel, q).start()
            if pn.rem:
                rem_copy(mask, sel, q).start()

    waiting = None
    for mask in masks:
        if mask:
            gather(mask)
            if waiting is None:
                pl.semaphore_wait(barrier, Q)
            else:
                send(waiting)
            waiting = mask
    own_copy.wait()
    send(waiting)
    cent_copy = remote(cents.at[side], cents.at[side], cs, cr, partner)
    cent_copy.start()
    cent_wait = remote(cents.at[other], cents.at[other], cs, cr, partner)
    gather_own()

    lanes = table[...].astype(jnp.float32)
    entries = 2 * pn.blocks
    entry_row = to_column(lanes[0:1], 0, entries)
    entry_lane = to_column(lanes[1:2], 0, entries)
    slot_home = to_column(lanes[2:3], 0, pn.slots)
    pick[...] = (entry_row == iota((entries, 8 * Q), 1).astype(jnp.float32)).astype(jnp.bfloat16)
    lane_group = (iota((entries, LANES), 1) // PB).astype(jnp.float32)
    pick_lane[...] = (entry_lane == lane_group).astype(jnp.float32)
    back[...] = (slot_home == iota((pn.slots, pn.blocks), 1).astype(jnp.float32)).astype(jnp.bfloat16)
    fill[...] = jnp.broadcast_to(jnp.where(slot_home < 0.0, FAR, 0.0), fill.shape)
    pmsg[...] = jnp.zeros_like(pmsg)
    lmsg[...] = jnp.zeros_like(lmsg)

    def set_norm(sel):
        wide = cents[sel].astype(jnp.float32)
        total = jnp.sum(wide * wide, axis=1, keepdims=True)
        norms[sel] = jnp.broadcast_to((inverse_root * LOG2E) * total, (CB, LANES))

    def tile_rows(sel, tile):
        block = recv[sel, pl.ds(tile * pn.tile_blocks, pn.tile_blocks)]
        return block.reshape(pn.tile_blocks * PB, pn.width)

    def score_tile(sel, tile):
        products = lax.dot_general(
            cents[sel], tile_rows(sel, tile), (((1,), (1,)), ((), ())),
            preferred_element_type=jnp.float32,
        )
        out = []
        for h in range(2):
            scores = (2.0 * inverse_root * LOG2E) * products[:, h * LANES : (h + 1) * LANES] - norms[sel]
            highest = jnp.max(scores, axis=0, keepdims=True)
            raised = jnp.exp2(scores - highest)
            escr[sel, 2 * tile + h] = raised
            mrow[pl.ds(sel * pn.groups + 2 * tile + h, 1)] = highest
            out.append(LN2 * highest + jnp.log(jnp.sum(raised, axis=0, keepdims=True)))
        return out

    def score_main(it, sel, tile):
        for h, part in enumerate(score_tile(sel, tile)):
            group = 2 * tile + h
            row = (group // pn.main_rows) * 8 + sel * pn.rows + group % pn.main_rows
            pmsg[it, pl.ds(row, 1)] = part

    main_tiles = Q * pn.main_rows // 2

    def score_rem(it, sel, tile):
        for h, part in enumerate(score_tile(sel, tile)):
            first = (2 * tile + h - Q * pn.main_rows) * pn.share
            for s in range(pn.share):
                row = (first + s) * 8 + sel * pn.rows + pn.main_rows
                pmsg[it, pl.ds(row, 1)] = part

    def score_all_rem(it, sel):
        @pl.loop(main_tiles, pn.tiles)
        def _(tile):
            score_rem(it, sel, tile)

    def trade(out, into, send_sem, recv_sem, it):
        into[it, pl.ds(q * 8, 8)] = out[it, pl.ds(q * 8, 8)]
        for mask in masks:
            if mask:
                spot = flip(q, mask)
                remote(
                    out.at[it, pl.ds(spot * 8, 8)], into.at[it, pl.ds(q * 8, 8)],
                    send_sem.at[it, mask], recv_sem.at[it, q], device(spot),
                ).start()
        for mask in masks:
            if mask:
                spot = flip(q, mask)
                copy = remote(
                    out.at[it, pl.ds(spot * 8, 8)], into.at[it, pl.ds(spot * 8, 8)],
                    send_sem.at[it, mask], recv_sem.at[it, spot], device(spot),
                )
                copy.wait()

    def combine(it):
        chosen = pick_rows(pick[...], split3(pin[it]))
        chosen = jnp.where(pick_lane[...] > 0.5, chosen, 0.0)
        step = LANES // 2
        while step >= PB:
            chosen = chosen + pltpu.roll(chosen, step, 1)
            step //= 2
        first, second = chosen[: pn.blocks], chosen[pn.blocks :]
        highest = jnp.maximum(first, second)
        lse = highest + jnp.log(jnp.exp(first - highest) + jnp.exp(second - highest))
        if it == ITERS - 1:
            grouped = lse.reshape(pn.blocks // GROUP, GROUP, LANES)
            shape = grouped.shape
            mine = iota(shape, 2) // PB == iota(shape, 1)
            lse_out[...] = jnp.sum(jnp.where(mine, grouped, 0.0), axis=1)
        spread = pick_rows(back[...], split3(lse)) + fill[...]
        lane = iota((2 * Q, LANES), 1) // PB
        for r in range(pn.rows):
            total = jnp.zeros((2 * Q, LANES), jnp.float32)
            for t in range(pn.cap):
                if (t // GROUP if t < pn.main else pn.main_rows) == r:
                    group = t % GROUP if t < pn.main else (q % pn.share) * pn.rem + t - pn.main
                    total = total + jnp.where(lane == group, spread[t * 2 * Q : (t + 1) * 2 * Q], 0.0)
            for sel in range(2):
                lmsg[it, pl.ds(sel * pn.rows + r, Q, stride=8)] = total[sel * Q : (sel + 1) * Q]

    def unpack(it):
        for sel in range(2):
            base = sel * pn.groups
            for r in range(pn.main_rows):
                rows = lin[it, pl.ds(sel * pn.rows + r, Q, stride=8)]
                if pn.main_rows == 1:
                    lrow[pl.ds(base, Q)] = rows
                else:
                    lrow[pl.ds(base + r, Q, stride=pn.main_rows)] = rows
            if pn.rem:
                rows = lin[it, pl.ds(sel * pn.rows + pn.main_rows, Q, stride=8)]
                joined = jnp.sum(rows.reshape(Q // pn.share, pn.share, LANES), axis=1)
                lrow[pl.ds(base + Q * pn.main_rows, Q // pn.share)] = joined

    def sum_up(sel):
        macc[...] = jnp.zeros_like(macc)
        rows = pn.tile_blocks * PB

        @pl.loop(0, pn.tiles, unroll=3)
        def _(tile):
            for h in range(2):
                row = sel * pn.groups + 2 * tile + h
                scale = jnp.exp2(mrow[pl.ds(row, 1)] - LOG2E * lrow[pl.ds(row, 1)])
                weights = escr[sel, 2 * tile + h] * scale
                macc[...] += weights
                wscr[:, pl.ds(pl.multiple_of(tile * rows + h * LANES, LANES), LANES)] = weights.astype(jnp.bfloat16)

        acc[...] = jnp.dot(
            wscr[...], recv[sel].reshape(pn.held * PB, pn.width), preferred_element_type=jnp.float32
        )
        return jnp.sum(macc[...], axis=1, keepdims=True)

    set_norm(side)
    cent_wait.wait_recv()
    set_norm(other)

    def wait_main(mask):
        spot = flip(q, mask)
        for sel in range(2):
            main_copy(mask, sel, spot).wait_recv()

    for pair in pn.pair_order()[-1:] + pn.pair_order()[:-1]:
        if pn.main:
            for low in (0, 1):
                if 2 * pair + low:
                    wait_main(2 * pair + low)
            if pn.main_rows == 1:
                tile = flip(q, 2 * pair) // 2

                for sel in range(2):
                    score_main(0, sel, tile)
    if pn.main_rows > 1:
        for sel in range(2):
            @pl.loop(0, main_tiles)
            def _(tile):
                score_main(0, sel, tile)
    if pn.rem:
        for mask in masks:
            if mask:
                for sel in range(2):
                    rem_copy(mask, sel, flip(q, mask)).wait_recv()
        for sel in range(2):
            score_all_rem(0, sel)
    trade(pmsg, pin, ps, pr, 0)
    combine(0)
    trade(lmsg, lin, ls, lr, 0)
    unpack(0)

    def x_copy(sel):
        return remote(xout.at[sel], xin.at[sel], xs.at[sel], xr.at[sel], partner)

    def m_copy(sel):
        return remote(mout.at[sel], min_.at[sel], ms.at[sel], mr.at[sel], partner)

    for sel in (other, side):
        mass = sum_up(sel)
        mout[sel] = jnp.broadcast_to(to_row(mass), (8, CB))
        xout[sel] = acc[...].astype(jnp.bfloat16)
        m_copy(sel).start()
        x_copy(sel).start()

    def renewed(sums, mass, old):
        return ((sums + old.astype(jnp.float32)) / (mass + 1.0)).astype(jnp.bfloat16)

    cent_copy.wait_send()
    for sel in (side, other):
        m_copy(sel).wait_recv()
        x_copy(sel).wait_recv()
        mass = to_column(mout[sel][0:1] + min_[sel][0:1], 0, CB)
        both = xout[sel].astype(jnp.float32) + xin[sel].astype(jnp.float32)
        cents[sel] = renewed(both, mass, cents[sel])
        set_norm(sel)
        if pn.main:
            @pl.loop(0, main_tiles, unroll=2)
            def _(tile):
                score_main(1, sel, tile)
        if pn.rem:
            score_all_rem(1, sel)

    trade(pmsg, pin, ps, pr, 1)
    combine(1)
    trade(lmsg, lin, ls, lr, 1)
    unpack(1)
    rows = CB // CHUNKS

    def x2_copy(k):
        part = pl.ds(k * rows, rows)
        return remote(xout2.at[part], xin2.at[part], x2s.at[k], x2r.at[k], partner)

    m2_copy = remote(mout2, min2, m2s, m2r, partner)
    mass = sum_up(other)
    mout2[...] = jnp.broadcast_to(to_row(mass), (8, CB))
    xout2[...] = acc[...].astype(jnp.bfloat16)
    m2_copy.start()
    for k in range(CHUNKS):
        x2_copy(k).start()
    mass = sum_up(side)
    m2_copy.wait_recv()
    mass = mass + to_column(min2[0:1], 0, CB)

    def f_copy(step, k, spot):
        part = new_out.at[spot, pl.ds(k * rows, rows)]
        to = {"pts": p, "cent": (c + step) % pn.cent}
        return remote(part, part, fs.at[step, k], fr.at[spot, k], to)

    for k in range(CHUNKS):
        part = pl.ds(k * rows, rows)
        x2_copy(k).wait_recv()
        sums = acc[part] + xin2[part].astype(jnp.float32)
        new_out[c, part] = renewed(sums, mass[k * rows : (k + 1) * rows], cents[side, part])
        for step in range(1, pn.cent):
            f_copy(step, k, c).start()

    for mask in masks:
        if mask:
            for sel in range(2):
                if pn.main:
                    main_copy(mask, sel, q).wait_send()
                if pn.rem:
                    rem_copy(mask, sel, q).wait_send()
    for sel in range(2):
        m_copy(sel).wait_send()
        x_copy(sel).wait_send()
    m2_copy.wait_send()
    for k in range(CHUNKS):
        x2_copy(k).wait_send()
        for step in range(1, pn.cent):
            f_copy(step, k, c).wait_send()
            f_copy(step, k, (c - step + pn.cent) % pn.cent).wait_recv()


def tables(pn, candidates):
    q = (lax.axis_index("pts") % pn.half) * pn.cent + lax.axis_index("cent")
    picked = candidates.T.reshape(-1)
    count = picked.shape[0]
    index = jnp.arange(count, dtype=jnp.int32)
    labels = jnp.arange(pn.total, dtype=jnp.int32)
    member = (picked[:, None] == labels[None, :]).astype(jnp.bfloat16)
    earlier = (index[None, :] < index[:, None]).astype(jnp.bfloat16)
    prior = jnp.dot(earlier, member, preferred_element_type=jnp.float32)
    turn = jnp.sum(prior * member.astype(jnp.float32), axis=1).astype(jnp.int32)
    place = picked * pn.cap + turn
    spot, sel = picked % pn.spots, picked // pn.spots
    in_main = turn < pn.main
    row = spot * 8 + sel * pn.rows + jnp.where(in_main, turn // GROUP, pn.main_rows)
    lane = jnp.where(in_main, turn % GROUP, (q % pn.share) * pn.rem + turn - pn.main)
    places = jnp.arange(pn.slots, dtype=jnp.int32)
    block = index % pn.blocks
    source = jnp.sum(jnp.where(place[:, None] == places[None, :], block[:, None] + 1, 0), axis=0) - 1
    by_turn = source.reshape(pn.total, pn.cap).T.reshape(-1)
    width = -(-max(count, pn.slots) // LANES) * LANES

    def row_of(values):
        return jnp.pad(values, (0, width - values.shape[0]))[None]

    rows = jnp.concatenate([row_of(row), row_of(lane), row_of(by_turn)], axis=0)
    table = jnp.pad(rows, ((0, 5), (0, 0)))
    return jnp.maximum(source, 0), table


def on_device(points, centroids, candidates):
    width = points.shape[1]
    pn = Plan(lax.axis_size("pts"), lax.axis_size("cent"), candidates.shape[0], width)
    assert centroids.shape[0] == pn.cent * CB
    home, table = tables(pn, candidates)
    Q, bf16, f32 = pn.spots, jnp.bfloat16, jnp.float32
    vmem = pl.BlockSpec(memory_space=pltpu.VMEM)
    dma = pltpu.SemaphoreType.DMA
    buffers = [
        ((Q, 2, pn.cap, PB, width), bf16),
        ((2, pn.held, PB, width), bf16),
        ((2, CB, width), bf16),
        ((2, CB, LANES), f32),
        ((2, pn.groups, CB, LANES), f32),
        ((CB, pn.held * PB), bf16),
        ((2 * pn.groups, LANES), f32),
        ((2 * pn.groups, LANES), f32),
        ((CB, width), f32),
        ((CB, LANES), f32),
        ((2 * pn.blocks, 8 * Q), bf16),
        ((2 * pn.blocks, LANES), f32),
        ((pn.slots, pn.blocks), bf16),
        ((pn.slots, LANES), f32),
        ((ITERS, 8 * Q, LANES), f32),
        ((ITERS, 8 * Q, LANES), f32),
        ((ITERS, 8 * Q, LANES), f32),
        ((ITERS, 8 * Q, LANES), f32),
        ((2, CB, width), bf16),
        ((2, CB, width), bf16),
        ((2, 8, CB), f32),
        ((2, 8, CB), f32),
        ((CB, width), bf16),
        ((CB, width), bf16),
        ((8, CB), f32),
        ((8, CB), f32),
    ]
    taken = sum(math.prod(shape) * jnp.dtype(kind).itemsize for shape, kind in buffers)
    new, lse = pl.pallas_call(
        functools.partial(kernel, pn, 1.0 / math.sqrt(width)),
        out_shape=(
            jax.ShapeDtypeStruct((pn.cent, CB, width), bf16),
            jax.ShapeDtypeStruct((pn.blocks // GROUP, LANES), f32),
        ),
        in_specs=[pl.BlockSpec(memory_space=pltpu.SMEM), vmem, vmem, pl.BlockSpec(memory_space=pl.ANY)],
        out_specs=(vmem, vmem),
        scratch_shapes=[pltpu.VMEM(*buffer) for buffer in buffers] + [
            dma((Q, 2)), dma((Q, 2)), dma((Q, 2)), dma((Q, 2)),
            dma, dma, dma,
            dma((ITERS, Q)), dma((ITERS, Q)), dma((ITERS, Q)), dma((ITERS, Q)),
            dma((2,)), dma((2,)), dma((2,)), dma((2,)),
            dma((CHUNKS,)), dma((CHUNKS,)), dma, dma,
            dma((pn.cent, CHUNKS)), dma((pn.cent, CHUNKS)),
        ],
        compiler_params=pltpu.CompilerParams(
            collective_id=0, has_side_effects=True, vmem_limit_bytes=taken + SPARE
        ),
    )(home, table, points.reshape(pn.blocks, PB, width), centroids.reshape(pn.cent, CB, width))
    return new.reshape(centroids.shape), lse.reshape(-1)


def solution(mesh):
    return jax.shard_map(
        on_device,
        mesh=mesh,
        in_specs=(P(("pts", "cent"), None), P("pts", None), P(("pts", "cent"), None)),
        out_specs=(P("pts", None), P(("pts", "cent"))),
        check_vma=False,
    )
```

```python
import functools
import math

import jax
import jax.numpy as jnp
from jax import lax
from jax.experimental import pallas as pl
from jax.experimental.pallas import tpu as pltpu
from jax.sharding import PartitionSpec as P

CB = 256
PB = 16
ITERS = 2
LANES = 128
GROUP = LANES // PB
CHUNKS = 8
SPARE = 12 << 20
LOG2E = math.log2(math.e)
LN2 = math.log(2.0)
MESH = pl.DeviceIdType.MESH
FAR = 1e30


class Plan:
    def __init__(self, pts, cent, point_blocks, width):
        self.pts, self.cent, self.blocks, self.width = pts, cent, point_blocks, width
        self.half = pts // 2
        self.spots = self.half * cent
        self.total = 2 * self.spots
        self.cap = max(2, 2 * point_blocks // self.total + 1)
        self.main = self.cap // GROUP * GROUP
        self.rem = self.cap - self.main
        self.main_rows = self.main // GROUP
        self.rows = self.main_rows + (self.rem > 0)
        self.share = GROUP // self.rem if self.rem else 1
        self.slots = self.total * self.cap
        self.held = self.spots * self.cap
        self.groups = self.held // GROUP
        self.tiles = self.groups // 2
        self.tile_blocks = 2 * GROUP
        assert GROUP % max(self.rem, 1) == 0 and 2 * self.rows <= 8
        assert self.spots & (self.spots - 1) == 0 and self.held % self.tile_blocks == 0

    def pair_order(self):
        pairs = self.spots // 2
        if pairs == 8:
            return (7, 3, 4, 5, 2, 1, 6, 0)
        return tuple(reversed(range(pairs)))


def flip(value, mask):
    out, bit = 0, 1
    while bit <= mask or bit == 1:
        here = (value // bit) % 2
        out = out + bit * ((1 - here) if mask & bit else here)
        bit *= 2
    return out + (value // bit) * bit


def split3(x):
    hi = x.astype(jnp.bfloat16)
    left = x - hi.astype(jnp.float32)
    mid = left.astype(jnp.bfloat16)
    low = (left - mid.astype(jnp.float32)).astype(jnp.bfloat16)
    return jnp.concatenate([hi, mid, low], axis=1)


def pick_rows(onehot, packed):
    out = jnp.dot(onehot, packed, preferred_element_type=jnp.float32)
    return (out[:, :LANES] + out[:, LANES : 2 * LANES]) + out[:, 2 * LANES :]


def iota(shape, axis):
    return lax.broadcasted_iota(jnp.int32, shape, axis)


def to_column(row, start, size):
    parts = []
    for first in range(0, size, LANES):
        part = min(LANES, size - first)
        piece = row[:, start + first : start + first + LANES]
        same = iota((part, LANES), 0) == iota((part, LANES), 1)
        parts.append(jnp.sum(jnp.where(same, piece, 0.0), axis=1, keepdims=True))
    return jnp.concatenate(parts, axis=0)


def to_row(column):
    parts = []
    for first in range(0, column.shape[0], LANES):
        same = iota((LANES, LANES), 0) == iota((LANES, LANES), 1)
        parts.append(jnp.sum(jnp.where(same, column[first : first + LANES], 0.0), axis=0, keepdims=True))
    return jnp.concatenate(parts, axis=1)


def kernel(
    pn, inverse_root, named_in, points_in, cent_in, new_out, lse_out,
    named, points, home_v, home, stage, recv, cents, norms, escr, wscr, mrow, lrow, acc, macc,
    pick, pick_lane, back, fill,
    pmsg, pin, lmsg, lin, xout, xin, mout, min_, xout2, xin2, mout2, min2,
    named_sem, pts_sem, home_sem, main_s, main_r, rem_s, rem_r, cent_sem, cs, cr, ps, pr, ls, lr,
    xs, xr, ms, mr, x2s, x2r, m2s, m2r, fs, fr,
):
    p, c = lax.axis_index("pts"), lax.axis_index("cent")
    side = p // pn.half
    other = 1 - side
    q = (p % pn.half) * pn.cent + c
    Q = pn.spots

    def device(spot):
        return {"pts": side * pn.half + spot // pn.cent, "cent": spot % pn.cent}

    partner = {"pts": other * pn.half + p % pn.half, "cent": c}

    def remote(src, dst, send, recv_sem, to):
        return pltpu.make_async_remote_copy(
            src_ref=src, dst_ref=dst, send_sem=send, recv_sem=recv_sem,
            device_id=to, device_id_type=MESH,
        )

    named_copy = pltpu.make_async_copy(named_in, named, named_sem)
    named_copy.start()
    parts = pn.blocks // 4
    point_copies = [
        pltpu.make_async_copy(
            points_in.at[pl.ds(k * parts, parts)], points.at[pl.ds(k * parts, parts)], pts_sem.at[k]
        )
        for k in range(4)
    ]
    for copy in point_copies:
        copy.start()
    own_copy = pltpu.make_async_copy(cent_in.at[c], cents.at[side], cent_sem)
    own_copy.start()

    barrier = pltpu.get_barrier_semaphore()
    for mask in range(1, Q):
        pl.semaphore_signal(barrier, inc=1, device_id=device(flip(q, mask)), device_id_type=MESH)
    pl.semaphore_signal(barrier, inc=1, device_id=partner, device_id_type=MESH)
    named_copy.wait()

    entries = 2 * pn.blocks
    picked = jnp.concatenate([named[0:1], named[1:2]], axis=1).astype(jnp.float32)
    member = picked == iota((pn.total, entries), 0).astype(jnp.float32)
    earlier = (iota((entries, entries), 0) < iota((entries, entries), 1)).astype(jnp.bfloat16)
    prior = jnp.dot(member.astype(jnp.bfloat16), earlier, preferred_element_type=jnp.float32)
    turn = jnp.sum(jnp.where(member, prior, 0.0), axis=0, keepdims=True)
    holder = iota((pn.total, entries), 1) % pn.blocks + 1
    homes = [
        jnp.sum(jnp.where(member & (turn == float(t)), holder, 0).astype(jnp.float32), axis=1, keepdims=True) - 1.0
        for t in range(pn.cap)
    ]
    grid = jnp.zeros((pn.total, LANES), jnp.int32)
    for t in range(pn.cap):
        grid = jnp.where(iota(grid.shape, 1) == t, jnp.maximum(homes[t], 0.0).astype(jnp.int32), grid)
    home_v[...] = grid
    home_copy = pltpu.make_async_copy(home_v, home, home_sem)

    masks = [2 * pair + low for pair in pn.pair_order() for low in (0, 1)]

    def point_block(block, t):
        return points[jnp.clip(home[block, t], 0, pn.blocks - 1)]

    def gather(mask):
        spot = flip(q, mask)
        for sel in range(2):
            for t in range(pn.cap):
                stage[mask, sel, t] = point_block(sel * Q + spot, t)

    def gather_own():
        for sel in range(2):
            for t in range(pn.main):
                recv[sel, q * pn.main + t] = point_block(sel * Q + q, t)
            for t in range(pn.rem):
                recv[sel, Q * pn.main + q * pn.rem + t] = point_block(sel * Q + q, pn.main + t)

    def main_copy(mask, sel, spot_at):
        return remote(
            stage.at[mask, sel, pl.ds(0, pn.main)],
            recv.at[sel, pl.ds(spot_at * pn.main, pn.main)],
            main_s.at[mask, sel], main_r.at[spot_at, sel], device(flip(q, mask)),
        )

    def rem_copy(mask, sel, spot_at):
        return remote(
            stage.at[mask, sel, pl.ds(pn.main, pn.rem)],
            recv.at[sel, pl.ds(Q * pn.main + spot_at * pn.rem, pn.rem)],
            rem_s.at[mask, sel], rem_r.at[spot_at, sel], device(flip(q, mask)),
        )

    def send(mask):
        for sel in range(2):
            if pn.main:
                main_copy(mask, sel, q).start()
            if pn.rem:
                rem_copy(mask, sel, q).start()

    for copy in point_copies:
        copy.wait()
    home_copy.start()
    home_copy.wait()
    waiting = None
    for mask in masks:
        if mask:
            gather(mask)
            if waiting is None:
                pl.semaphore_wait(barrier, Q)
            else:
                send(waiting)
            waiting = mask
    own_copy.wait()
    send(waiting)
    cent_copy = remote(cents.at[side], cents.at[side], cs, cr, partner)
    cent_copy.start()
    cent_wait = remote(cents.at[other], cents.at[other], cs, cr, partner)
    gather_own()

    upper = (picked >= float(Q)).astype(jnp.float32)
    spot_row = picked - float(Q) * upper
    eighth = jnp.floor(turn * (1.0 / GROUP))
    in_main = turn < float(pn.main)
    row = spot_row * 8.0 + upper * float(pn.rows) + jnp.where(in_main, eighth, float(pn.main_rows))
    mine = ((q % pn.share) * pn.rem - pn.main).astype(jnp.float32)
    lane = jnp.where(in_main, turn - GROUP * eighth, turn + mine)
    entry_row = to_column(row, 0, entries)
    entry_lane = to_column(lane, 0, entries)
    slot_home = jnp.concatenate(homes, axis=0)
    pick[...] = (entry_row == iota((entries, 8 * Q), 1).astype(jnp.float32)).astype(jnp.bfloat16)
    lane_group = (iota((entries, LANES), 1) // PB).astype(jnp.float32)
    pick_lane[...] = (entry_lane == lane_group).astype(jnp.float32)
    back[...] = (slot_home == iota((pn.slots, pn.blocks), 1).astype(jnp.float32)).astype(jnp.bfloat16)
    fill[...] = jnp.broadcast_to(jnp.where(slot_home < 0.0, FAR, 0.0), fill.shape)
    pmsg[...] = jnp.zeros_like(pmsg)
    lmsg[...] = jnp.zeros_like(lmsg)

    def set_norm(sel):
        wide = cents[sel].astype(jnp.float32)
        total = jnp.sum(wide * wide, axis=1, keepdims=True)
        norms[sel] = jnp.broadcast_to((inverse_root * LOG2E) * total, (CB, LANES))

    def tile_rows(sel, tile):
        block = recv[sel, pl.ds(tile * pn.tile_blocks, pn.tile_blocks)]
        return block.reshape(pn.tile_blocks * PB, pn.width)

    def score_tile(sel, tile):
        products = lax.dot_general(
            cents[sel], tile_rows(sel, tile), (((1,), (1,)), ((), ())),
            preferred_element_type=jnp.float32,
        )
        out = []
        for h in range(2):
            scores = (2.0 * inverse_root * LOG2E) * products[:, h * LANES : (h + 1) * LANES] - norms[sel]
            highest = jnp.max(scores, axis=0, keepdims=True)
            raised = jnp.exp2(scores - highest)
            escr[sel, 2 * tile + h] = raised
            mrow[pl.ds(sel * pn.groups + 2 * tile + h, 1)] = highest
            out.append(LN2 * highest + jnp.log(jnp.sum(raised, axis=0, keepdims=True)))
        return out

    def score_main(it, sel, tile):
        for h, part in enumerate(score_tile(sel, tile)):
            group = 2 * tile + h
            row = (group // pn.main_rows) * 8 + sel * pn.rows + group % pn.main_rows
            pmsg[it, pl.ds(row, 1)] = part

    main_tiles = Q * pn.main_rows // 2

    def score_rem(it, sel, tile):
        for h, part in enumerate(score_tile(sel, tile)):
            first = (2 * tile + h - Q * pn.main_rows) * pn.share
            for s in range(pn.share):
                row = (first + s) * 8 + sel * pn.rows + pn.main_rows
                pmsg[it, pl.ds(row, 1)] = part

    def score_all_rem(it, sel):
        @pl.loop(main_tiles, pn.tiles)
        def _(tile):
            score_rem(it, sel, tile)

    def trade(out, into, send_sem, recv_sem, it):
        into[it, pl.ds(q * 8, 8)] = out[it, pl.ds(q * 8, 8)]
        for mask in masks:
            if mask:
                spot = flip(q, mask)
                remote(
                    out.at[it, pl.ds(spot * 8, 8)], into.at[it, pl.ds(q * 8, 8)],
                    send_sem.at[it, mask], recv_sem.at[it, q], device(spot),
                ).start()
        for mask in masks:
            if mask:
                spot = flip(q, mask)
                copy = remote(
                    out.at[it, pl.ds(spot * 8, 8)], into.at[it, pl.ds(spot * 8, 8)],
                    send_sem.at[it, mask], recv_sem.at[it, spot], device(spot),
                )
                copy.wait()

    def combine(it):
        chosen = pick_rows(pick[...], split3(pin[it]))
        chosen = jnp.where(pick_lane[...] > 0.5, chosen, 0.0)
        step = LANES // 2
        while step >= PB:
            chosen = chosen + pltpu.roll(chosen, step, 1)
            step //= 2
        first, second = chosen[: pn.blocks], chosen[pn.blocks :]
        highest = jnp.maximum(first, second)
        lse = highest + jnp.log(jnp.exp(first - highest) + jnp.exp(second - highest))
        if it == ITERS - 1:
            grouped = lse.reshape(pn.blocks // GROUP, GROUP, LANES)
            shape = grouped.shape
            mine = iota(shape, 2) // PB == iota(shape, 1)
            lse_out[...] = jnp.sum(jnp.where(mine, grouped, 0.0), axis=1)
        spread = pick_rows(back[...], split3(lse)) + fill[...]
        lane = iota((2 * Q, LANES), 1) // PB
        for r in range(pn.rows):
            total = jnp.zeros((2 * Q, LANES), jnp.float32)
            for t in range(pn.cap):
                if (t // GROUP if t < pn.main else pn.main_rows) == r:
                    group = t % GROUP if t < pn.main else (q % pn.share) * pn.rem + t - pn.main
                    total = total + jnp.where(lane == group, spread[t * 2 * Q : (t + 1) * 2 * Q], 0.0)
            for sel in range(2):
                lmsg[it, pl.ds(sel * pn.rows + r, Q, stride=8)] = total[sel * Q : (sel + 1) * Q]

    def unpack(it):
        for sel in range(2):
            base = sel * pn.groups
            for r in range(pn.main_rows):
                rows = lin[it, pl.ds(sel * pn.rows + r, Q, stride=8)]
                if pn.main_rows == 1:
                    lrow[pl.ds(base, Q)] = rows
                else:
                    lrow[pl.ds(base + r, Q, stride=pn.main_rows)] = rows
            if pn.rem:
                rows = lin[it, pl.ds(sel * pn.rows + pn.main_rows, Q, stride=8)]
                joined = jnp.sum(rows.reshape(Q // pn.share, pn.share, LANES), axis=1)
                lrow[pl.ds(base + Q * pn.main_rows, Q // pn.share)] = joined

    def sum_up(sel):
        macc[...] = jnp.zeros_like(macc)
        rows = pn.tile_blocks * PB

        @pl.loop(0, pn.tiles, unroll=3)
        def _(tile):
            for h in range(2):
                row = sel * pn.groups + 2 * tile + h
                scale = jnp.exp2(mrow[pl.ds(row, 1)] - LOG2E * lrow[pl.ds(row, 1)])
                weights = escr[sel, 2 * tile + h] * scale
                macc[...] += weights
                wscr[:, pl.ds(pl.multiple_of(tile * rows + h * LANES, LANES), LANES)] = weights.astype(jnp.bfloat16)

        acc[...] = jnp.dot(
            wscr[...], recv[sel].reshape(pn.held * PB, pn.width), preferred_element_type=jnp.float32
        )
        return jnp.sum(macc[...], axis=1, keepdims=True)

    set_norm(side)
    cent_wait.wait_recv()
    set_norm(other)

    def wait_main(mask):
        spot = flip(q, mask)
        for sel in range(2):
            main_copy(mask, sel, spot).wait_recv()

    for pair in pn.pair_order()[-1:] + pn.pair_order()[:-1]:
        if pn.main:
            for low in (0, 1):
                if 2 * pair + low:
                    wait_main(2 * pair + low)
            if pn.main_rows == 1:
                tile = flip(q, 2 * pair) // 2

                for sel in range(2):
                    score_main(0, sel, tile)
    if pn.main_rows > 1:
        for sel in range(2):
            @pl.loop(0, main_tiles)
            def _(tile):
                score_main(0, sel, tile)
    if pn.rem:
        for mask in masks:
            if mask:
                for sel in range(2):
                    rem_copy(mask, sel, flip(q, mask)).wait_recv()
        for sel in range(2):
            score_all_rem(0, sel)
    trade(pmsg, pin, ps, pr, 0)
    combine(0)
    trade(lmsg, lin, ls, lr, 0)
    unpack(0)

    def x_copy(sel):
        return remote(xout.at[sel], xin.at[sel], xs.at[sel], xr.at[sel], partner)

    def m_copy(sel):
        return remote(mout.at[sel], min_.at[sel], ms.at[sel], mr.at[sel], partner)

    for sel in (other, side):
        mass = sum_up(sel)
        mout[sel] = jnp.broadcast_to(to_row(mass), (8, CB))
        xout[sel] = acc[...].astype(jnp.bfloat16)
        m_copy(sel).start()
        x_copy(sel).start()

    def renewed(sums, mass, old):
        return ((sums + old.astype(jnp.float32)) / (mass + 1.0)).astype(jnp.bfloat16)

    cent_copy.wait_send()
    for sel in (side, other):
        m_copy(sel).wait_recv()
        x_copy(sel).wait_recv()
        mass = to_column(mout[sel][0:1] + min_[sel][0:1], 0, CB)
        both = xout[sel].astype(jnp.float32) + xin[sel].astype(jnp.float32)
        cents[sel] = renewed(both, mass, cents[sel])
        set_norm(sel)
        if pn.main:
            @pl.loop(0, main_tiles, unroll=2)
            def _(tile):
                score_main(1, sel, tile)
        if pn.rem:
            score_all_rem(1, sel)

    trade(pmsg, pin, ps, pr, 1)
    combine(1)
    trade(lmsg, lin, ls, lr, 1)
    unpack(1)
    rows = CB // CHUNKS

    def x2_copy(k):
        part = pl.ds(k * rows, rows)
        return remote(xout2.at[part], xin2.at[part], x2s.at[k], x2r.at[k], partner)

    m2_copy = remote(mout2, min2, m2s, m2r, partner)
    mass = sum_up(other)
    mout2[...] = jnp.broadcast_to(to_row(mass), (8, CB))
    xout2[...] = acc[...].astype(jnp.bfloat16)
    m2_copy.start()
    for k in range(CHUNKS):
        x2_copy(k).start()
    mass = sum_up(side)
    m2_copy.wait_recv()
    mass = mass + to_column(min2[0:1], 0, CB)

    def f_copy(step, k, spot):
        part = new_out.at[spot, pl.ds(k * rows, rows)]
        to = {"pts": p, "cent": (c + step) % pn.cent}
        return remote(part, part, fs.at[step, k], fr.at[spot, k], to)

    for k in range(CHUNKS):
        part = pl.ds(k * rows, rows)
        x2_copy(k).wait_recv()
        sums = acc[part] + xin2[part].astype(jnp.float32)
        new_out[c, part] = renewed(sums, mass[k * rows : (k + 1) * rows], cents[side, part])
        for step in range(1, pn.cent):
            f_copy(step, k, c).start()

    for mask in masks:
        if mask:
            for sel in range(2):
                if pn.main:
                    main_copy(mask, sel, q).wait_send()
                if pn.rem:
                    rem_copy(mask, sel, q).wait_send()
    for sel in range(2):
        m_copy(sel).wait_send()
        x_copy(sel).wait_send()
    m2_copy.wait_send()
    for k in range(CHUNKS):
        x2_copy(k).wait_send()
        for step in range(1, pn.cent):
            f_copy(step, k, c).wait_send()
            f_copy(step, k, (c - step + pn.cent) % pn.cent).wait_recv()


def on_device(points, centroids, candidates):
    width = points.shape[1]
    pn = Plan(lax.axis_size("pts"), lax.axis_size("cent"), candidates.shape[0], width)
    assert centroids.shape[0] == pn.cent * CB
    Q, bf16, f32 = pn.spots, jnp.bfloat16, jnp.float32
    vmem = pl.BlockSpec(memory_space=pltpu.VMEM)
    hbm = pl.BlockSpec(memory_space=pltpu.HBM)
    dma = pltpu.SemaphoreType.DMA
    early = [((2, pn.blocks), jnp.int32), ((pn.blocks, PB, width), bf16), ((pn.total, LANES), jnp.int32)]
    buffers = [
        ((Q, 2, pn.cap, PB, width), bf16),
        ((2, pn.held, PB, width), bf16),
        ((2, CB, width), bf16),
        ((2, CB, LANES), f32),
        ((2, pn.groups, CB, LANES), f32),
        ((CB, pn.held * PB), bf16),
        ((2 * pn.groups, LANES), f32),
        ((2 * pn.groups, LANES), f32),
        ((CB, width), f32),
        ((CB, LANES), f32),
        ((2 * pn.blocks, 8 * Q), bf16),
        ((2 * pn.blocks, LANES), f32),
        ((pn.slots, pn.blocks), bf16),
        ((pn.slots, LANES), f32),
        ((ITERS, 8 * Q, LANES), f32),
        ((ITERS, 8 * Q, LANES), f32),
        ((ITERS, 8 * Q, LANES), f32),
        ((ITERS, 8 * Q, LANES), f32),
        ((2, CB, width), bf16),
        ((2, CB, width), bf16),
        ((2, 8, CB), f32),
        ((2, 8, CB), f32),
        ((CB, width), bf16),
        ((CB, width), bf16),
        ((8, CB), f32),
        ((8, CB), f32),
    ]
    taken = sum(math.prod(shape) * jnp.dtype(kind).itemsize for shape, kind in early + buffers)
    new, lse = pl.pallas_call(
        functools.partial(kernel, pn, 1.0 / math.sqrt(width)),
        out_shape=(
            jax.ShapeDtypeStruct((pn.cent, CB, width), bf16),
            jax.ShapeDtypeStruct((pn.blocks // GROUP, LANES), f32),
        ),
        in_specs=[hbm, hbm, hbm],
        out_specs=(vmem, vmem),
        scratch_shapes=[pltpu.VMEM(*buffer) for buffer in early]
        + [pltpu.SMEM((pn.total, LANES), jnp.int32)]
        + [pltpu.VMEM(*buffer) for buffer in buffers]
        + [
            dma, dma((4,)), dma,
            dma((Q, 2)), dma((Q, 2)), dma((Q, 2)), dma((Q, 2)),
            dma, dma, dma,
            dma((ITERS, Q)), dma((ITERS, Q)), dma((ITERS, Q)), dma((ITERS, Q)),
            dma((2,)), dma((2,)), dma((2,)), dma((2,)),
            dma((CHUNKS,)), dma((CHUNKS,)), dma, dma,
            dma((pn.cent, CHUNKS)), dma((pn.cent, CHUNKS)),
        ],
        compiler_params=pltpu.CompilerParams(
            collective_id=0, has_side_effects=True, vmem_limit_bytes=taken + SPARE
        ),
    )(
        pltpu.with_memory_space_constraint(candidates.T, pltpu.HBM),
        pltpu.with_memory_space_constraint(points.reshape(pn.blocks, PB, width), pltpu.HBM),
        pltpu.with_memory_space_constraint(centroids.reshape(pn.cent, CB, width), pltpu.HBM),
    )
    return new.reshape(centroids.shape), lse.reshape(-1)


def solution(mesh):
    return jax.shard_map(
        on_device,
        mesh=mesh,
        in_specs=(P(("pts", "cent"), None), P("pts", None), P(("pts", "cent"), None)),
        out_specs=(P("pts", None), P(("pts", "cent"))),
        check_vma=False,
    )
```

```python
import functools
import math

import jax
import jax.numpy as jnp
from jax import lax
from jax.experimental import pallas as pl
from jax.experimental.pallas import tpu as pltpu
from jax.sharding import PartitionSpec as P

CB = 256
PB = 16
ITERS = 2
LANES = 128
GROUP = LANES // PB
CHUNKS = 8
SPARE = 12 << 20
LOG2E = math.log2(math.e)
LN2 = math.log(2.0)
MESH = pl.DeviceIdType.MESH
FAR = 1e30


class Plan:
    def __init__(self, pts, cent, point_blocks, width):
        self.pts, self.cent, self.blocks, self.width = pts, cent, point_blocks, width
        self.half = pts // 2
        self.spots = self.half * cent
        self.total = 2 * self.spots
        self.cap = max(2, 2 * point_blocks // self.total + 1)
        self.main = self.cap // GROUP * GROUP
        self.rem = self.cap - self.main
        self.main_rows = self.main // GROUP
        self.rows = self.main_rows + (self.rem > 0)
        self.share = GROUP // self.rem if self.rem else 1
        self.slots = self.total * self.cap
        self.held = self.spots * self.cap
        self.groups = self.held // GROUP
        self.tiles = self.groups // 2
        self.tile_blocks = 2 * GROUP
        assert GROUP % max(self.rem, 1) == 0 and 2 * self.rows <= 8
        assert self.cent % 2 == 0 and self.spots & (self.spots - 1) == 0 and self.held % self.tile_blocks == 0

    def pair_order(self):
        pairs = self.spots // 2
        if pairs == 8:
            return (7, 3, 4, 5, 2, 1, 6, 0)
        return tuple(reversed(range(pairs)))


def flip(value, mask):
    out, bit = 0, 1
    while bit <= mask or bit == 1:
        here = (value // bit) % 2
        out = out + bit * ((1 - here) if mask & bit else here)
        bit *= 2
    return out + (value // bit) * bit


def split3(x):
    hi = x.astype(jnp.bfloat16)
    left = x - hi.astype(jnp.float32)
    mid = left.astype(jnp.bfloat16)
    low = (left - mid.astype(jnp.float32)).astype(jnp.bfloat16)
    return jnp.concatenate([hi, mid, low], axis=1)


def pick_rows(onehot, packed):
    out = jnp.dot(onehot, packed, preferred_element_type=jnp.float32)
    return (out[:, :LANES] + out[:, LANES : 2 * LANES]) + out[:, 2 * LANES :]


def iota(shape, axis):
    return lax.broadcasted_iota(jnp.int32, shape, axis)


def to_column(row, start, size):
    parts = []
    for first in range(0, size, LANES):
        part = min(LANES, size - first)
        piece = row[:, start + first : start + first + LANES]
        same = iota((part, LANES), 0) == iota((part, LANES), 1)
        parts.append(jnp.sum(jnp.where(same, piece, 0.0), axis=1, keepdims=True))
    return jnp.concatenate(parts, axis=0)


def to_row(column):
    parts = []
    for first in range(0, column.shape[0], LANES):
        same = iota((LANES, LANES), 0) == iota((LANES, LANES), 1)
        parts.append(jnp.sum(jnp.where(same, column[first : first + LANES], 0.0), axis=0, keepdims=True))
    return jnp.concatenate(parts, axis=1)


def kernel(
    pn, inverse_root, named_in, points_in, cent_in, new_out, lse_out,
    named, points, home_v, home, stage, recv, cents, norms, escr, wscr, mrow, lrow, acc, macc,
    pick, pick_lane, back, fill,
    pmsg, pin, lmsg, lin, xout, xin, mout, min_, xout2, xin2, mout2, min2,
    named_sem, pts_sem, home_sem, main_s, main_r, rem_s, rem_r, cent_sem, cs, cr, ps, pr, ls, lr,
    xs, xr, ms, mr, x2s, x2r, m2s, m2r, fs, fr,
):
    p, c = lax.axis_index("pts"), lax.axis_index("cent")
    side = p // pn.half
    other = 1 - side
    q = (p % pn.half) * pn.cent + c
    Q = pn.spots

    def device(spot):
        return {"pts": side * pn.half + spot // pn.cent, "cent": spot % pn.cent}

    partner = {"pts": other * pn.half + p % pn.half, "cent": c}

    def remote(src, dst, send, recv_sem, to):
        return pltpu.make_async_remote_copy(
            src_ref=src, dst_ref=dst, send_sem=send, recv_sem=recv_sem,
            device_id=to, device_id_type=MESH,
        )

    named_copy = pltpu.make_async_copy(named_in, named, named_sem)
    named_copy.start()
    parts = pn.blocks // 4
    point_copies = [
        pltpu.make_async_copy(
            points_in.at[pl.ds(k * parts, parts)], points.at[pl.ds(k * parts, parts)], pts_sem.at[k]
        )
        for k in range(4)
    ]
    for copy in point_copies:
        copy.start()
    own_copy = pltpu.make_async_copy(cent_in.at[c], cents.at[side], cent_sem)
    own_copy.start()

    barrier = pltpu.get_barrier_semaphore()
    for mask in range(1, Q):
        pl.semaphore_signal(barrier, inc=1, device_id=device(flip(q, mask)), device_id_type=MESH)
    pl.semaphore_signal(barrier, inc=1, device_id=partner, device_id_type=MESH)
    named_copy.wait()

    entries = 2 * pn.blocks
    picked = jnp.concatenate([named[0:1], named[1:2]], axis=1).astype(jnp.float32)
    member = picked == iota((pn.total, entries), 0).astype(jnp.float32)
    earlier = (iota((entries, entries), 0) < iota((entries, entries), 1)).astype(jnp.bfloat16)
    prior = jnp.dot(member.astype(jnp.bfloat16), earlier, preferred_element_type=jnp.float32)
    turn = jnp.sum(jnp.where(member, prior, 0.0), axis=0, keepdims=True)
    holder = iota((pn.total, entries), 1) % pn.blocks + 1
    homes = [
        jnp.sum(jnp.where(member & (turn == float(t)), holder, 0).astype(jnp.float32), axis=1, keepdims=True) - 1.0
        for t in range(pn.cap)
    ]
    grid = jnp.zeros((pn.total, LANES), jnp.int32)
    for t in range(pn.cap):
        grid = jnp.where(iota(grid.shape, 1) == t, jnp.maximum(homes[t], 0.0).astype(jnp.int32), grid)
    home_v[...] = grid
    home_copy = pltpu.make_async_copy(home_v, home, home_sem)

    masks = [2 * pair + low for pair in pn.pair_order() for low in (0, 1)]

    def point_block(block, t):
        return points[jnp.clip(home[block, t], 0, pn.blocks - 1)]

    def gather(mask):
        spot = flip(q, mask)
        for sel in range(2):
            for t in range(pn.cap):
                stage[mask, sel, t] = point_block(sel * Q + spot, t)

    def gather_own():
        for sel in range(2):
            for t in range(pn.main):
                recv[sel, q * pn.main + t] = point_block(sel * Q + q, t)
            for t in range(pn.rem):
                recv[sel, Q * pn.main + q * pn.rem + t] = point_block(sel * Q + q, pn.main + t)

    def main_copy(mask, sel, spot_at):
        return remote(
            stage.at[mask, sel, pl.ds(0, pn.main)],
            recv.at[sel, pl.ds(spot_at * pn.main, pn.main)],
            main_s.at[mask, sel], main_r.at[spot_at, sel], device(flip(q, mask)),
        )

    def rem_copy(mask, sel, spot_at):
        return remote(
            stage.at[mask, sel, pl.ds(pn.main, pn.rem)],
            recv.at[sel, pl.ds(Q * pn.main + spot_at * pn.rem, pn.rem)],
            rem_s.at[mask, sel], rem_r.at[spot_at, sel], device(flip(q, mask)),
        )

    def send(mask):
        for sel in range(2):
            if pn.main:
                main_copy(mask, sel, q).start()
            if pn.rem:
                rem_copy(mask, sel, q).start()

    for copy in point_copies:
        copy.wait()
    home_copy.start()
    home_copy.wait()
    waiting = None
    for mask in masks:
        if mask:
            gather(mask)
            if waiting is None:
                pl.semaphore_wait(barrier, Q)
            else:
                send(waiting)
            waiting = mask
    own_copy.wait()
    send(waiting)
    cent_copy = remote(cents.at[side], cents.at[side], cs, cr, partner)
    cent_copy.start()
    cent_wait = remote(cents.at[other], cents.at[other], cs, cr, partner)
    gather_own()

    upper = (picked >= float(Q)).astype(jnp.float32)
    spot_row = picked - float(Q) * upper
    eighth = jnp.floor(turn * (1.0 / GROUP))
    in_main = turn < float(pn.main)
    row = spot_row * 8.0 + upper * float(pn.rows) + jnp.where(in_main, eighth, float(pn.main_rows))
    mine = ((q % pn.share) * pn.rem - pn.main).astype(jnp.float32)
    lane = jnp.where(in_main, turn - GROUP * eighth, turn + mine)
    entry_row = to_column(row, 0, entries)
    entry_lane = to_column(lane, 0, entries)
    slot_home = jnp.concatenate(homes, axis=0)
    pick[...] = (entry_row == iota((entries, 8 * Q), 1).astype(jnp.float32)).astype(jnp.bfloat16)
    lane_group = (iota((entries, LANES), 1) // PB).astype(jnp.float32)
    pick_lane[...] = (entry_lane == lane_group).astype(jnp.float32)
    back[...] = (slot_home == iota((pn.slots, pn.blocks), 1).astype(jnp.float32)).astype(jnp.bfloat16)
    fill[...] = jnp.broadcast_to(jnp.where(slot_home < 0.0, FAR, 0.0), fill.shape)
    pmsg[...] = jnp.zeros_like(pmsg)
    lmsg[...] = jnp.zeros_like(lmsg)

    def set_norm(sel):
        wide = cents[sel].astype(jnp.float32)
        total = jnp.sum(wide * wide, axis=1, keepdims=True)
        norms[sel] = jnp.broadcast_to((inverse_root * LOG2E) * total, (CB, LANES))

    def tile_rows(sel, tile):
        block = recv[sel, pl.ds(tile * pn.tile_blocks, pn.tile_blocks)]
        return block.reshape(pn.tile_blocks * PB, pn.width)

    def score_tile(sel, tile):
        products = lax.dot_general(
            cents[sel], tile_rows(sel, tile), (((1,), (1,)), ((), ())),
            preferred_element_type=jnp.float32,
        )
        out = []
        for h in range(2):
            scores = (2.0 * inverse_root * LOG2E) * products[:, h * LANES : (h + 1) * LANES] - norms[sel]
            highest = jnp.max(scores, axis=0, keepdims=True)
            raised = jnp.exp2(scores - highest)
            escr[sel, 2 * tile + h] = raised
            mrow[pl.ds(sel * pn.groups + 2 * tile + h, 1)] = highest
            out.append(LN2 * highest + jnp.log(jnp.sum(raised, axis=0, keepdims=True)))
        return out

    def score_main(it, sel, tile):
        for h, part in enumerate(score_tile(sel, tile)):
            group = 2 * tile + h
            row = (group // pn.main_rows) * 8 + sel * pn.rows + group % pn.main_rows
            pmsg[it, pl.ds(row, 1)] = part

    main_tiles = Q * pn.main_rows // 2

    def score_rem(it, sel, tile):
        for h, part in enumerate(score_tile(sel, tile)):
            first = (2 * tile + h - Q * pn.main_rows) * pn.share
            for s in range(pn.share):
                row = (first + s) * 8 + sel * pn.rows + pn.main_rows
                pmsg[it, pl.ds(row, 1)] = part

    def trade(out, into, send_sem, recv_sem, it):
        into[it, pl.ds(q * 8, 8)] = out[it, pl.ds(q * 8, 8)]
        for mask in masks:
            if mask:
                spot = flip(q, mask)
                remote(
                    out.at[it, pl.ds(spot * 8, 8)], into.at[it, pl.ds(q * 8, 8)],
                    send_sem.at[it, mask], recv_sem.at[it, q], device(spot),
                ).start()
        for mask in masks:
            if mask:
                spot = flip(q, mask)
                copy = remote(
                    out.at[it, pl.ds(spot * 8, 8)], into.at[it, pl.ds(spot * 8, 8)],
                    send_sem.at[it, mask], recv_sem.at[it, spot], device(spot),
                )
                copy.wait()

    def combine(it):
        chosen = pick_rows(pick[...], split3(pin[it]))
        chosen = jnp.where(pick_lane[...] > 0.5, chosen, 0.0)
        step = LANES // 2
        while step >= PB:
            chosen = chosen + pltpu.roll(chosen, step, 1)
            step //= 2
        first, second = chosen[: pn.blocks], chosen[pn.blocks :]
        highest = jnp.maximum(first, second)
        lse = highest + jnp.log(jnp.exp(first - highest) + jnp.exp(second - highest))
        if it == ITERS - 1:
            grouped = lse.reshape(pn.blocks // GROUP, GROUP, LANES)
            shape = grouped.shape
            mine = iota(shape, 2) // PB == iota(shape, 1)
            lse_out[...] = jnp.sum(jnp.where(mine, grouped, 0.0), axis=1)
        spread = pick_rows(back[...], split3(lse)) + fill[...]
        lane = iota((2 * Q, LANES), 1) // PB
        for r in range(pn.rows):
            total = jnp.zeros((2 * Q, LANES), jnp.float32)
            for t in range(pn.cap):
                if (t // GROUP if t < pn.main else pn.main_rows) == r:
                    group = t % GROUP if t < pn.main else (q % pn.share) * pn.rem + t - pn.main
                    total = total + jnp.where(lane == group, spread[t * 2 * Q : (t + 1) * 2 * Q], 0.0)
            for sel in range(2):
                lmsg[it, pl.ds(sel * pn.rows + r, Q, stride=8)] = total[sel * Q : (sel + 1) * Q]

    def unpack(it):
        for sel in range(2):
            base = sel * pn.groups
            for r in range(pn.main_rows):
                rows = lin[it, pl.ds(sel * pn.rows + r, Q, stride=8)]
                if pn.main_rows == 1:
                    lrow[pl.ds(base, Q)] = rows
                else:
                    lrow[pl.ds(base + r, Q, stride=pn.main_rows)] = rows
            if pn.rem:
                rows = lin[it, pl.ds(sel * pn.rows + pn.main_rows, Q, stride=8)]
                joined = jnp.sum(rows.reshape(Q // pn.share, pn.share, LANES), axis=1)
                lrow[pl.ds(base + Q * pn.main_rows, Q // pn.share)] = joined

    def sum_up(sel):
        macc[...] = jnp.zeros_like(macc)
        rows = pn.tile_blocks * PB

        @pl.loop(0, pn.tiles, unroll=3)
        def _(tile):
            for h in range(2):
                row = sel * pn.groups + 2 * tile + h
                scale = jnp.exp2(mrow[pl.ds(row, 1)] - LOG2E * lrow[pl.ds(row, 1)])
                weights = escr[sel, 2 * tile + h] * scale
                macc[...] += weights
                wscr[:, pl.ds(pl.multiple_of(tile * rows + h * LANES, LANES), LANES)] = weights.astype(jnp.bfloat16)

        acc[...] = jnp.dot(
            wscr[...], recv[sel].reshape(pn.held * PB, pn.width), preferred_element_type=jnp.float32
        )
        return jnp.sum(macc[...], axis=1, keepdims=True)

    set_norm(side)
    cent_wait.wait_recv()
    set_norm(other)

    def score_all(it, sel):
        for tile in range(pn.tiles):
            (score_main if tile < main_tiles else score_rem)(it, sel, tile)

    for mask in masks:
        if mask:
            for sel in range(2):
                if pn.main:
                    main_copy(mask, sel, flip(q, mask)).wait_recv()
                if pn.rem:
                    rem_copy(mask, sel, flip(q, mask)).wait_recv()
    for sel in range(2):
        score_all(0, sel)
    trade(pmsg, pin, ps, pr, 0)
    combine(0)
    trade(lmsg, lin, ls, lr, 0)
    unpack(0)

    def x_copy(sel):
        return remote(xout.at[sel], xin.at[sel], xs.at[sel], xr.at[sel], partner)

    def m_copy(sel):
        return remote(mout.at[sel], min_.at[sel], ms.at[sel], mr.at[sel], partner)

    for sel in (other, side):
        mass = sum_up(sel)
        mout[sel] = jnp.broadcast_to(to_row(mass), (8, CB))
        xout[sel] = acc[...].astype(jnp.bfloat16)
        m_copy(sel).start()
        x_copy(sel).start()

    def renewed(sums, mass, old):
        return ((sums + old.astype(jnp.float32)) / (mass + 1.0)).astype(jnp.bfloat16)

    cent_copy.wait_send()
    for sel in (side, other):
        m_copy(sel).wait_recv()
        x_copy(sel).wait_recv()
        mass = to_column(mout[sel][0:1] + min_[sel][0:1], 0, CB)
        both = xout[sel].astype(jnp.float32) + xin[sel].astype(jnp.float32)
        cents[sel] = renewed(both, mass, cents[sel])
        set_norm(sel)
        score_all(1, sel)

    trade(pmsg, pin, ps, pr, 1)
    combine(1)
    trade(lmsg, lin, ls, lr, 1)
    unpack(1)
    rows = CB // CHUNKS

    def x2_copy(k):
        part = pl.ds(k * rows, rows)
        return remote(xout2.at[part], xin2.at[part], x2s.at[k], x2r.at[k], partner)

    m2_copy = remote(mout2, min2, m2s, m2r, partner)
    mass = sum_up(other)
    mout2[...] = jnp.broadcast_to(to_row(mass), (8, CB))
    xout2[...] = acc[...].astype(jnp.bfloat16)
    m2_copy.start()
    for k in range(CHUNKS):
        x2_copy(k).start()
    mass = sum_up(side)
    m2_copy.wait_recv()
    mass = mass + to_column(min2[0:1], 0, CB)

    pairs = pn.cent // 2
    beside = c + 1 - 2 * (c % 2)

    def away(step):
        return (c + 2 * step) % pn.cent

    def f_copy(number, k, spot, to):
        part = new_out.at[spot, pl.ds(k * rows, rows)]
        return remote(part, part, fs.at[number, k], fr.at[spot, k], {"pts": p, "cent": to})

    for k in range(CHUNKS):
        part = pl.ds(k * rows, rows)
        x2_copy(k).wait_recv()
        sums = acc[part] + xin2[part].astype(jnp.float32)
        new_out[c, part] = renewed(sums, mass[k * rows : (k + 1) * rows], cents[side, part])
        for step in range(1, pairs):
            f_copy(step, k, c, away(step)).start()
        f_copy(0, k, c, beside).start()
    for k in range(CHUNKS):
        for step in range(1, pairs):
            f_copy(step, k, away(pairs - step), c).wait_recv()
            f_copy(pairs + step - 1, k, away(pairs - step), beside).start()

    for mask in masks:
        if mask:
            for sel in range(2):
                if pn.main:
                    main_copy(mask, sel, q).wait_send()
                if pn.rem:
                    rem_copy(mask, sel, q).wait_send()
    for sel in range(2):
        m_copy(sel).wait_send()
        x_copy(sel).wait_send()
    m2_copy.wait_send()
    for k in range(CHUNKS):
        x2_copy(k).wait_send()
        f_copy(0, k, c, beside).wait_send()
        f_copy(0, k, beside, c).wait_recv()
        for step in range(1, pairs):
            f_copy(step, k, c, away(step)).wait_send()
            f_copy(pairs + step - 1, k, away(pairs - step), beside).wait_send()
            f_copy(0, k, (beside + 2 * (pairs - step)) % pn.cent, c).wait_recv()


def on_device(points, centroids, candidates):
    width = points.shape[1]
    pn = Plan(lax.axis_size("pts"), lax.axis_size("cent"), candidates.shape[0], width)
    assert centroids.shape[0] == pn.cent * CB
    Q, bf16, f32 = pn.spots, jnp.bfloat16, jnp.float32
    vmem = pl.BlockSpec(memory_space=pltpu.VMEM)
    hbm = pl.BlockSpec(memory_space=pltpu.HBM)
    dma = pltpu.SemaphoreType.DMA
    early = [((2, pn.blocks), jnp.int32), ((pn.blocks, PB, width), bf16), ((pn.total, LANES), jnp.int32)]
    buffers = [
        ((Q, 2, pn.cap, PB, width), bf16),
        ((2, pn.held, PB, width), bf16),
        ((2, CB, width), bf16),
        ((2, CB, LANES), f32),
        ((2, pn.groups, CB, LANES), f32),
        ((CB, pn.held * PB), bf16),
        ((2 * pn.groups, LANES), f32),
        ((2 * pn.groups, LANES), f32),
        ((CB, width), f32),
        ((CB, LANES), f32),
        ((2 * pn.blocks, 8 * Q), bf16),
        ((2 * pn.blocks, LANES), f32),
        ((pn.slots, pn.blocks), bf16),
        ((pn.slots, LANES), f32),
        ((ITERS, 8 * Q, LANES), f32),
        ((ITERS, 8 * Q, LANES), f32),
        ((ITERS, 8 * Q, LANES), f32),
        ((ITERS, 8 * Q, LANES), f32),
        ((2, CB, width), bf16),
        ((2, CB, width), bf16),
        ((2, 8, CB), f32),
        ((2, 8, CB), f32),
        ((CB, width), bf16),
        ((CB, width), bf16),
        ((8, CB), f32),
        ((8, CB), f32),
    ]
    taken = sum(math.prod(shape) * jnp.dtype(kind).itemsize for shape, kind in early + buffers)
    new, lse = pl.pallas_call(
        functools.partial(kernel, pn, 1.0 / math.sqrt(width)),
        out_shape=(
            jax.ShapeDtypeStruct((pn.cent, CB, width), bf16),
            jax.ShapeDtypeStruct((pn.blocks // GROUP, LANES), f32),
        ),
        in_specs=[hbm, hbm, hbm],
        out_specs=(vmem, vmem),
        scratch_shapes=[pltpu.VMEM(*buffer) for buffer in early]
        + [pltpu.SMEM((pn.total, LANES), jnp.int32)]
        + [pltpu.VMEM(*buffer) for buffer in buffers]
        + [
            dma, dma((4,)), dma,
            dma((Q, 2)), dma((Q, 2)), dma((Q, 2)), dma((Q, 2)),
            dma, dma, dma,
            dma((ITERS, Q)), dma((ITERS, Q)), dma((ITERS, Q)), dma((ITERS, Q)),
            dma((2,)), dma((2,)), dma((2,)), dma((2,)),
            dma((CHUNKS,)), dma((CHUNKS,)), dma, dma,
            dma((pn.cent, CHUNKS)), dma((pn.cent, CHUNKS)),
        ],
        compiler_params=pltpu.CompilerParams(
            collective_id=0, has_side_effects=True, vmem_limit_bytes=taken + SPARE
        ),
    )(
        pltpu.with_memory_space_constraint(candidates.T, pltpu.HBM),
        pltpu.with_memory_space_constraint(points.reshape(pn.blocks, PB, width), pltpu.HBM),
        pltpu.with_memory_space_constraint(centroids.reshape(pn.cent, CB, width), pltpu.HBM),
    )
    return new.reshape(centroids.shape), lse.reshape(-1)


def solution(mesh):
    return jax.shard_map(
        on_device,
        mesh=mesh,
        in_specs=(P(("pts", "cent"), None), P("pts", None), P(("pts", "cent"), None)),
        out_specs=(P("pts", None), P(("pts", "cent"))),
        check_vma=False,
    )
```

```python
import functools
import math

import jax
import jax.numpy as jnp
from jax import lax
from jax.experimental import pallas as pl
from jax.experimental.pallas import tpu as pltpu
from jax.sharding import PartitionSpec as P

CB = 256
PB = 16
ITERS = 2
LANES = 128
GROUP = LANES // PB
CHUNKS = 8
SPARE = 12 << 20
LOG2E = math.log2(math.e)
LN2 = math.log(2.0)
MESH = pl.DeviceIdType.MESH
FAR = 1e30


class Plan:
    def __init__(self, pts, cent, point_blocks, width):
        self.pts, self.cent, self.blocks, self.width = pts, cent, point_blocks, width
        self.half = pts // 2
        self.spots = self.half * cent
        self.total = 2 * self.spots
        self.cap = max(2, 2 * point_blocks // self.total + 1)
        self.main = self.cap // GROUP * GROUP
        self.rem = self.cap - self.main
        self.main_rows = self.main // GROUP
        self.rows = self.main_rows + (self.rem > 0)
        self.share = GROUP // self.rem if self.rem else 1
        self.slots = self.total * self.cap
        self.held = self.spots * self.cap
        self.groups = self.held // GROUP
        self.tiles = self.groups // 2
        self.tile_blocks = 2 * GROUP
        assert GROUP % max(self.rem, 1) == 0 and 2 * self.rows <= 8
        assert self.cent % 2 == 0 and self.spots & (self.spots - 1) == 0 and self.held % self.tile_blocks == 0

    def pair_order(self):
        pairs = self.spots // 2
        if pairs == 8:
            return (7, 3, 4, 5, 2, 1, 6, 0)
        return tuple(reversed(range(pairs)))


def flip(value, mask):
    out, bit = 0, 1
    while bit <= mask or bit == 1:
        here = (value // bit) % 2
        out = out + bit * ((1 - here) if mask & bit else here)
        bit *= 2
    return out + (value // bit) * bit


def split3(x):
    hi = x.astype(jnp.bfloat16)
    left = x - hi.astype(jnp.float32)
    mid = left.astype(jnp.bfloat16)
    low = (left - mid.astype(jnp.float32)).astype(jnp.bfloat16)
    return jnp.concatenate([hi, mid, low], axis=1)


def pick_rows(onehot, packed):
    out = jnp.dot(onehot, packed, preferred_element_type=jnp.float32)
    return (out[:, :LANES] + out[:, LANES : 2 * LANES]) + out[:, 2 * LANES :]


def iota(shape, axis):
    return lax.broadcasted_iota(jnp.int32, shape, axis)


def to_column(row, start, size):
    parts = []
    for first in range(0, size, LANES):
        part = min(LANES, size - first)
        piece = row[:, start + first : start + first + LANES]
        same = iota((part, LANES), 0) == iota((part, LANES), 1)
        parts.append(jnp.sum(jnp.where(same, piece, 0.0), axis=1, keepdims=True))
    return jnp.concatenate(parts, axis=0)


def to_row(column):
    parts = []
    for first in range(0, column.shape[0], LANES):
        same = iota((LANES, LANES), 0) == iota((LANES, LANES), 1)
        parts.append(jnp.sum(jnp.where(same, column[first : first + LANES], 0.0), axis=0, keepdims=True))
    return jnp.concatenate(parts, axis=1)


def kernel(
    pn, inverse_root, named_in, points_in, cent_in, new_out, lse_out,
    named, points, home_v, home, stage, recv, cents, norms, escr, wscr, mrow, lrow, acc, macc,
    pick, pick_lane, back, fill,
    pmsg, pin, lmsg, lin, xout, xin, mout, min_, xout2, xin2, mout2, min2,
    named_sem, pts_sem, home_sem, main_s, main_r, rem_s, rem_r, cent_sem, cs, cr, ps, pr, ls, lr,
    xs, xr, ms, mr, x2s, x2r, m2s, m2r, fs, fr,
):
    p, c = lax.axis_index("pts"), lax.axis_index("cent")
    side = p // pn.half
    other = 1 - side
    q = (p % pn.half) * pn.cent + c
    Q = pn.spots

    def device(spot):
        return {"pts": side * pn.half + spot // pn.cent, "cent": spot % pn.cent}

    partner = {"pts": other * pn.half + p % pn.half, "cent": c}

    def remote(src, dst, send, recv_sem, to):
        return pltpu.make_async_remote_copy(
            src_ref=src, dst_ref=dst, send_sem=send, recv_sem=recv_sem,
            device_id=to, device_id_type=MESH,
        )

    named_copy = pltpu.make_async_copy(named_in, named, named_sem)
    named_copy.start()
    parts = pn.blocks // 4
    point_copies = [
        pltpu.make_async_copy(
            points_in.at[pl.ds(k * parts, parts)], points.at[pl.ds(k * parts, parts)], pts_sem.at[k]
        )
        for k in range(4)
    ]
    for copy in point_copies:
        copy.start()
    own_copy = pltpu.make_async_copy(cent_in.at[c], cents.at[side], cent_sem)
    own_copy.start()

    barrier = pltpu.get_barrier_semaphore()
    for mask in range(1, Q):
        pl.semaphore_signal(barrier, inc=1, device_id=device(flip(q, mask)), device_id_type=MESH)
    pl.semaphore_signal(barrier, inc=1, device_id=partner, device_id_type=MESH)
    named_copy.wait()

    entries = 2 * pn.blocks
    picked = jnp.concatenate([named[0:1], named[1:2]], axis=1).astype(jnp.float32)
    member = picked == iota((pn.total, entries), 0).astype(jnp.float32)
    earlier = (iota((entries, entries), 0) < iota((entries, entries), 1)).astype(jnp.bfloat16)
    prior = jnp.dot(member.astype(jnp.bfloat16), earlier, preferred_element_type=jnp.float32)
    turn = jnp.sum(jnp.where(member, prior, 0.0), axis=0, keepdims=True)
    holder = iota((pn.total, entries), 1) % pn.blocks + 1
    homes = [
        jnp.sum(jnp.where(member & (turn == float(t)), holder, 0).astype(jnp.float32), axis=1, keepdims=True) - 1.0
        for t in range(pn.cap)
    ]
    grid = jnp.zeros((pn.total, LANES), jnp.int32)
    for t in range(pn.cap):
        grid = jnp.where(iota(grid.shape, 1) == t, jnp.maximum(homes[t], 0.0).astype(jnp.int32), grid)
    home_v[...] = grid
    home_copy = pltpu.make_async_copy(home_v, home, home_sem)

    masks = [2 * pair + low for pair in pn.pair_order() for low in (0, 1)]

    def point_block(block, t):
        return points[jnp.clip(home[block, t], 0, pn.blocks - 1)]

    def gather(mask):
        spot = flip(q, mask)
        for sel in range(2):
            for t in range(pn.cap):
                stage[mask, sel, t] = point_block(sel * Q + spot, t)

    def gather_own():
        for sel in range(2):
            for t in range(pn.main):
                recv[sel, q * pn.main + t] = point_block(sel * Q + q, t)
            for t in range(pn.rem):
                recv[sel, Q * pn.main + q * pn.rem + t] = point_block(sel * Q + q, pn.main + t)

    def main_copy(mask, sel, spot_at):
        return remote(
            stage.at[mask, sel, pl.ds(0, pn.main)],
            recv.at[sel, pl.ds(spot_at * pn.main, pn.main)],
            main_s.at[mask, sel], main_r.at[spot_at, sel], device(flip(q, mask)),
        )

    def rem_copy(mask, sel, spot_at):
        return remote(
            stage.at[mask, sel, pl.ds(pn.main, pn.rem)],
            recv.at[sel, pl.ds(Q * pn.main + spot_at * pn.rem, pn.rem)],
            rem_s.at[mask, sel], rem_r.at[spot_at, sel], device(flip(q, mask)),
        )

    def send(mask):
        for sel in range(2):
            if pn.main:
                main_copy(mask, sel, q).start()
            if pn.rem:
                rem_copy(mask, sel, q).start()

    own_copy.wait()
    pl.semaphore_wait(barrier, Q)
    cent_copy = remote(cents.at[side], cents.at[side], cs, cr, partner)
    cent_copy.start()
    for copy in point_copies:
        copy.wait()
    home_copy.start()
    home_copy.wait()
    waiting = None
    for mask in masks:
        if mask:
            gather(mask)
            if waiting is not None:
                send(waiting)
            waiting = mask
    send(waiting)
    cent_wait = remote(cents.at[other], cents.at[other], cs, cr, partner)
    gather_own()

    upper = (picked >= float(Q)).astype(jnp.float32)
    spot_row = picked - float(Q) * upper
    eighth = jnp.floor(turn * (1.0 / GROUP))
    in_main = turn < float(pn.main)
    row = spot_row * 8.0 + upper * float(pn.rows) + jnp.where(in_main, eighth, float(pn.main_rows))
    mine = ((q % pn.share) * pn.rem - pn.main).astype(jnp.float32)
    lane = jnp.where(in_main, turn - GROUP * eighth, turn + mine)
    entry_row = to_column(row, 0, entries)
    entry_lane = to_column(lane, 0, entries)
    slot_home = jnp.concatenate(homes, axis=0)
    pick[...] = (entry_row == iota((entries, 8 * Q), 1).astype(jnp.float32)).astype(jnp.bfloat16)
    lane_group = (iota((entries, LANES), 1) // PB).astype(jnp.float32)
    pick_lane[...] = (entry_lane == lane_group).astype(jnp.float32)
    back[...] = (slot_home == iota((pn.slots, pn.blocks), 1).astype(jnp.float32)).astype(jnp.bfloat16)
    fill[...] = jnp.broadcast_to(jnp.where(slot_home < 0.0, FAR, 0.0), fill.shape)
    pmsg[...] = jnp.zeros_like(pmsg)
    lmsg[...] = jnp.zeros_like(lmsg)

    def set_norm(sel):
        wide = cents[sel].astype(jnp.float32)
        total = jnp.sum(wide * wide, axis=1, keepdims=True)
        norms[sel] = jnp.broadcast_to((inverse_root * LOG2E) * total, (CB, LANES))

    def tile_rows(sel, tile):
        block = recv[sel, pl.ds(tile * pn.tile_blocks, pn.tile_blocks)]
        return block.reshape(pn.tile_blocks * PB, pn.width)

    def score_tile(sel, tile):
        products = lax.dot_general(
            cents[sel], tile_rows(sel, tile), (((1,), (1,)), ((), ())),
            preferred_element_type=jnp.float32,
        )
        out = []
        for h in range(2):
            scores = (2.0 * inverse_root * LOG2E) * products[:, h * LANES : (h + 1) * LANES] - norms[sel]
            highest = jnp.max(scores, axis=0, keepdims=True)
            raised = jnp.exp2(scores - highest)
            escr[sel, 2 * tile + h] = raised
            mrow[pl.ds(sel * pn.groups + 2 * tile + h, 1)] = highest
            out.append(LN2 * highest + jnp.log(jnp.sum(raised, axis=0, keepdims=True)))
        return out

    def score_main(it, sel, tile):
        for h, part in enumerate(score_tile(sel, tile)):
            group = 2 * tile + h
            row = (group // pn.main_rows) * 8 + sel * pn.rows + group % pn.main_rows
            pmsg[it, pl.ds(row, 1)] = part

    main_tiles = Q * pn.main_rows // 2

    def score_rem(it, sel, tile):
        for h, part in enumerate(score_tile(sel, tile)):
            first = (2 * tile + h - Q * pn.main_rows) * pn.share
            for s in range(pn.share):
                row = (first + s) * 8 + sel * pn.rows + pn.main_rows
                pmsg[it, pl.ds(row, 1)] = part

    def trade(out, into, send_sem, recv_sem, it):
        into[it, pl.ds(q * 8, 8)] = out[it, pl.ds(q * 8, 8)]
        for mask in masks:
            if mask:
                spot = flip(q, mask)
                remote(
                    out.at[it, pl.ds(spot * 8, 8)], into.at[it, pl.ds(q * 8, 8)],
                    send_sem.at[it, mask], recv_sem.at[it, q], device(spot),
                ).start()
        for mask in masks:
            if mask:
                spot = flip(q, mask)
                copy = remote(
                    out.at[it, pl.ds(spot * 8, 8)], into.at[it, pl.ds(spot * 8, 8)],
                    send_sem.at[it, mask], recv_sem.at[it, spot], device(spot),
                )
                copy.wait()

    def combine(it):
        chosen = pick_rows(pick[...], split3(pin[it]))
        chosen = jnp.where(pick_lane[...] > 0.5, chosen, 0.0)
        step = LANES // 2
        while step >= PB:
            chosen = chosen + pltpu.roll(chosen, step, 1)
            step //= 2
        first, second = chosen[: pn.blocks], chosen[pn.blocks :]
        highest = jnp.maximum(first, second)
        lse = highest + jnp.log(jnp.exp(first - highest) + jnp.exp(second - highest))
        if it == ITERS - 1:
            grouped = lse.reshape(pn.blocks // GROUP, GROUP, LANES)
            shape = grouped.shape
            mine = iota(shape, 2) // PB == iota(shape, 1)
            lse_out[...] = jnp.sum(jnp.where(mine, grouped, 0.0), axis=1)
        spread = pick_rows(back[...], split3(lse)) + fill[...]
        lane = iota((2 * Q, LANES), 1) // PB
        for r in range(pn.rows):
            total = jnp.zeros((2 * Q, LANES), jnp.float32)
            for t in range(pn.cap):
                if (t // GROUP if t < pn.main else pn.main_rows) == r:
                    group = t % GROUP if t < pn.main else (q % pn.share) * pn.rem + t - pn.main
                    total = total + jnp.where(lane == group, spread[t * 2 * Q : (t + 1) * 2 * Q], 0.0)
            for sel in range(2):
                lmsg[it, pl.ds(sel * pn.rows + r, Q, stride=8)] = total[sel * Q : (sel + 1) * Q]

    def unpack(it):
        for sel in range(2):
            base = sel * pn.groups
            for r in range(pn.main_rows):
                rows = lin[it, pl.ds(sel * pn.rows + r, Q, stride=8)]
                if pn.main_rows == 1:
                    lrow[pl.ds(base, Q)] = rows
                else:
                    lrow[pl.ds(base + r, Q, stride=pn.main_rows)] = rows
            if pn.rem:
                rows = lin[it, pl.ds(sel * pn.rows + pn.main_rows, Q, stride=8)]
                joined = jnp.sum(rows.reshape(Q // pn.share, pn.share, LANES), axis=1)
                lrow[pl.ds(base + Q * pn.main_rows, Q // pn.share)] = joined

    def sum_up(sel):
        macc[...] = jnp.zeros_like(macc)
        rows = pn.tile_blocks * PB

        @pl.loop(0, pn.tiles, unroll=3)
        def _(tile):
            for h in range(2):
                row = sel * pn.groups + 2 * tile + h
                scale = jnp.exp2(mrow[pl.ds(row, 1)] - LOG2E * lrow[pl.ds(row, 1)])
                weights = escr[sel, 2 * tile + h] * scale
                macc[...] += weights
                wscr[:, pl.ds(pl.multiple_of(tile * rows + h * LANES, LANES), LANES)] = weights.astype(jnp.bfloat16)

        acc[...] = jnp.dot(
            wscr[...], recv[sel].reshape(pn.held * PB, pn.width), preferred_element_type=jnp.float32
        )
        return jnp.sum(macc[...], axis=1, keepdims=True)

    set_norm(side)
    cent_wait.wait_recv()
    set_norm(other)

    def score_all(it, sel):
        for tile in range(pn.tiles):
            (score_main if tile < main_tiles else score_rem)(it, sel, tile)

    for mask in masks:
        if mask:
            for sel in range(2):
                if pn.main:
                    main_copy(mask, sel, flip(q, mask)).wait_recv()
                if pn.rem:
                    rem_copy(mask, sel, flip(q, mask)).wait_recv()
    for sel in range(2):
        score_all(0, sel)
    trade(pmsg, pin, ps, pr, 0)
    combine(0)
    trade(lmsg, lin, ls, lr, 0)
    unpack(0)

    def x_copy(sel):
        return remote(xout.at[sel], xin.at[sel], xs.at[sel], xr.at[sel], partner)

    def m_copy(sel):
        return remote(mout.at[sel], min_.at[sel], ms.at[sel], mr.at[sel], partner)

    for sel in (other, side):
        mass = sum_up(sel)
        mout[sel] = jnp.broadcast_to(to_row(mass), (8, CB))
        xout[sel] = acc[...].astype(jnp.bfloat16)
        m_copy(sel).start()
        x_copy(sel).start()

    def renewed(sums, mass, old):
        return ((sums + old.astype(jnp.float32)) / (mass + 1.0)).astype(jnp.bfloat16)

    cent_copy.wait_send()
    for sel in (side, other):
        m_copy(sel).wait_recv()
        x_copy(sel).wait_recv()
        mass = to_column(mout[sel][0:1] + min_[sel][0:1], 0, CB)
        both = xout[sel].astype(jnp.float32) + xin[sel].astype(jnp.float32)
        cents[sel] = renewed(both, mass, cents[sel])
        set_norm(sel)
        score_all(1, sel)

    trade(pmsg, pin, ps, pr, 1)
    combine(1)
    trade(lmsg, lin, ls, lr, 1)
    unpack(1)
    rows = CB // CHUNKS

    def x2_copy(k):
        part = pl.ds(k * rows, rows)
        return remote(xout2.at[part], xin2.at[part], x2s.at[k], x2r.at[k], partner)

    m2_copy = remote(mout2, min2, m2s, m2r, partner)
    mass = sum_up(other)
    mout2[...] = jnp.broadcast_to(to_row(mass), (8, CB))
    xout2[...] = acc[...].astype(jnp.bfloat16)
    m2_copy.start()
    for k in range(CHUNKS):
        x2_copy(k).start()
    mass = sum_up(side)
    m2_copy.wait_recv()
    mass = mass + to_column(min2[0:1], 0, CB)

    pairs = pn.cent // 2
    beside = c + 1 - 2 * (c % 2)

    def away(step):
        return (c + 2 * step) % pn.cent

    def f_copy(number, k, spot, to):
        part = new_out.at[spot, pl.ds(k * rows, rows)]
        return remote(part, part, fs.at[number, k], fr.at[spot, k], {"pts": p, "cent": to})

    for k in range(CHUNKS):
        part = pl.ds(k * rows, rows)
        x2_copy(k).wait_recv()
        sums = acc[part] + xin2[part].astype(jnp.float32)
        new_out[c, part] = renewed(sums, mass[k * rows : (k + 1) * rows], cents[side, part])
        for step in range(1, pairs):
            f_copy(step, k, c, away(step)).start()
        f_copy(0, k, c, beside).start()
    for k in range(CHUNKS):
        for step in range(1, pairs):
            f_copy(step, k, away(pairs - step), c).wait_recv()
            f_copy(pairs + step - 1, k, away(pairs - step), beside).start()

    for mask in masks:
        if mask:
            for sel in range(2):
                if pn.main:
                    main_copy(mask, sel, q).wait_send()
                if pn.rem:
                    rem_copy(mask, sel, q).wait_send()
    for sel in range(2):
        m_copy(sel).wait_send()
        x_copy(sel).wait_send()
    m2_copy.wait_send()
    for k in range(CHUNKS):
        x2_copy(k).wait_send()
        f_copy(0, k, c, beside).wait_send()
        f_copy(0, k, beside, c).wait_recv()
        for step in range(1, pairs):
            f_copy(step, k, c, away(step)).wait_send()
            f_copy(pairs + step - 1, k, away(pairs - step), beside).wait_send()
            f_copy(0, k, (beside + 2 * (pairs - step)) % pn.cent, c).wait_recv()


def on_device(points, centroids, candidates):
    width = points.shape[1]
    pn = Plan(lax.axis_size("pts"), lax.axis_size("cent"), candidates.shape[0], width)
    assert centroids.shape[0] == pn.cent * CB
    Q, bf16, f32 = pn.spots, jnp.bfloat16, jnp.float32
    vmem = pl.BlockSpec(memory_space=pltpu.VMEM)
    hbm = pl.BlockSpec(memory_space=pltpu.HBM)
    dma = pltpu.SemaphoreType.DMA
    early = [((2, pn.blocks), jnp.int32), ((pn.blocks, PB, width), bf16), ((pn.total, LANES), jnp.int32)]
    buffers = [
        ((Q, 2, pn.cap, PB, width), bf16),
        ((2, pn.held, PB, width), bf16),
        ((2, CB, width), bf16),
        ((2, CB, LANES), f32),
        ((2, pn.groups, CB, LANES), f32),
        ((CB, pn.held * PB), bf16),
        ((2 * pn.groups, LANES), f32),
        ((2 * pn.groups, LANES), f32),
        ((CB, width), f32),
        ((CB, LANES), f32),
        ((2 * pn.blocks, 8 * Q), bf16),
        ((2 * pn.blocks, LANES), f32),
        ((pn.slots, pn.blocks), bf16),
        ((pn.slots, LANES), f32),
        ((ITERS, 8 * Q, LANES), f32),
        ((ITERS, 8 * Q, LANES), f32),
        ((ITERS, 8 * Q, LANES), f32),
        ((ITERS, 8 * Q, LANES), f32),
        ((2, CB, width), bf16),
        ((2, CB, width), bf16),
        ((2, 8, CB), f32),
        ((2, 8, CB), f32),
        ((CB, width), bf16),
        ((CB, width), bf16),
        ((8, CB), f32),
        ((8, CB), f32),
    ]
    taken = sum(math.prod(shape) * jnp.dtype(kind).itemsize for shape, kind in early + buffers)
    new, lse = pl.pallas_call(
        functools.partial(kernel, pn, 1.0 / math.sqrt(width)),
        out_shape=(
            jax.ShapeDtypeStruct((pn.cent, CB, width), bf16),
            jax.ShapeDtypeStruct((pn.blocks // GROUP, LANES), f32),
        ),
        in_specs=[hbm, hbm, hbm],
        out_specs=(vmem, vmem),
        scratch_shapes=[pltpu.VMEM(*buffer) for buffer in early]
        + [pltpu.SMEM((pn.total, LANES), jnp.int32)]
        + [pltpu.VMEM(*buffer) for buffer in buffers]
        + [
            dma, dma((4,)), dma,
            dma((Q, 2)), dma((Q, 2)), dma((Q, 2)), dma((Q, 2)),
            dma, dma, dma,
            dma((ITERS, Q)), dma((ITERS, Q)), dma((ITERS, Q)), dma((ITERS, Q)),
            dma((2,)), dma((2,)), dma((2,)), dma((2,)),
            dma((CHUNKS,)), dma((CHUNKS,)), dma, dma,
            dma((pn.cent, CHUNKS)), dma((pn.cent, CHUNKS)),
        ],
        compiler_params=pltpu.CompilerParams(
            collective_id=0, has_side_effects=True, vmem_limit_bytes=taken + SPARE
        ),
    )(
        pltpu.with_memory_space_constraint(candidates.T, pltpu.HBM),
        pltpu.with_memory_space_constraint(points.reshape(pn.blocks, PB, width), pltpu.HBM),
        pltpu.with_memory_space_constraint(centroids.reshape(pn.cent, CB, width), pltpu.HBM),
    )
    return new.reshape(centroids.shape), lse.reshape(-1)


def solution(mesh):
    return jax.shard_map(
        on_device,
        mesh=mesh,
        in_specs=(P(("pts", "cent"), None), P("pts", None), P(("pts", "cent"), None)),
        out_specs=(P("pts", None), P(("pts", "cent"))),
        check_vma=False,
    )
```
